128 devices in a mesh: tm: 32 (over z_lo, x, y), panel: 4 (over z_hi, core).
Axes of the slice: x: 4, y: 4, z: 4 (z_hi: 2, z_lo: 2; z = z_hi * 2 + z_lo), core: 2. Of those that a mesh axis runs over, the one named last changes fastest.
Arguments:
- series: float32 [48, 8192], P(None, 'tm'), may hold values from -20 to 20, as said below
- start_block: float32 [18432, 64], P(('tm', 'panel')), may hold values from -6 to 6
Outputs:
- covariance: float32 [18432, 18432], P(('tm', 'panel'))
- basis: float32 [7, 18432, 64], P(None, ('tm', 'panel'))
- diag_blocks: float32 [6, 64, 64], replicated
- off_blocks: float32 [7, 64, 64], replicated
The draws below stay inside these ranges and needn't reach their ends.
Inputs may be any that keep to these rules, and one draw needn't show every extreme that they name: `series`: each channel has its own scale.
All inputs are finite; a program needn't handle non-finite values.
Results may differ from the reference program's by a relative error of at most 0.0003.
Values sent between devices are 32-bit elements; how exact they have to be, the bound alone decides.
A program may use at most 128 MiB of HBM per device.

```python
import math
import jax
import jax.numpy as jnp
from jax import lax

L = 48
M = 384
B = 64
ITERS = 6
NT = 8192
LM = 18432


def draw_series(key, part):
    scale_key = jax.random.fold_in(key, 11)
    noise_key = jax.random.fold_in(key, 12)
    scales = jnp.exp(jax.random.uniform(scale_key, (L, 1), jnp.float32, math.log(0.3), math.log(3.0)))
    noise = jnp.clip(jax.random.normal(noise_key, (L, NT), jnp.float32), -6.0, 6.0)
    return (scales * noise).astype(jnp.float32)


def block_levels(rng, dims, split, low, top_value):
    def one(axis_at, blocks):
        draws = jax.random.uniform(jax.random.fold_in(jax.random.fold_in(rng, 6), axis_at), (blocks,), jnp.float32, low / len(split), top_value / len(split))
        return jnp.repeat(jnp.exp(draws), dims[axis_at] // blocks).reshape((-1,) + (1,) * (len(dims) - axis_at - 1))

    factor_of = one(*split[0])
    for cut in split[1:]:
        factor_of = factor_of * one(*cut)
    return factor_of


def centred(rng, shape, scale, limit, split=(), kind=jnp.bfloat16):
    array = scale * jax.random.normal(rng, shape, jnp.float32)
    if split:
        array = array * block_levels(rng, shape, split, -0.22, 0.18)
    return jnp.clip(array, -limit, limit).astype(kind)


def setup_inputs(seed: int = 0) -> dict:
    seeds = jax.random.split(jax.random.key(seed), 3)
    return {
        "series": draw_series(jax.random.fold_in(seeds[2], 71), 0),
        "start_block": centred(seeds[1], (LM, B), 1.0, 6.0, ((0, 128),), jnp.float32),
    }


exact_precision = lax.Precision.HIGHEST

def lower_factor(gram_matrix):
    return jnp.linalg.cholesky(gram_matrix)

def reference(series, start_block):
    padded = jnp.concatenate([series, jnp.zeros((L, M), jnp.float32)], axis=1)

    def one_lag(lag_index):
        shifted = lax.dynamic_slice(padded, (jnp.int32(0), lag_index.astype(jnp.int32)), (L, NT))
        return jnp.dot(series.astype(jnp.float32), shifted.T.astype(jnp.float32), precision=exact_precision, preferred_element_type=jnp.float32)
    lag_sums = lax.map(one_lag, jnp.arange(M, dtype=jnp.int32))
    lag_sums = jnp.transpose(lag_sums, (1, 0, 2))
    counts = (NT - jnp.arange(M)).astype(jnp.float32)
    normed = lag_sums / counts[None, :, None]
    two_sided = jnp.concatenate([jnp.transpose(normed, (2, 1, 0))[:, :0:-1, :], normed], axis=1)

    def one_row(lag_index):
        window = lax.dynamic_slice(two_sided, (jnp.int32(0), (M - 1 - lag_index).astype(jnp.int32), jnp.int32(0)), (L, M, L))
        return window.reshape(L, M * L)
    covariance = lax.map(one_row, jnp.arange(M, dtype=jnp.int32)).reshape(M * L, M * L)
    factor = lower_factor(jnp.dot(start_block.T.astype(jnp.float32), start_block.astype(jnp.float32), precision=exact_precision, preferred_element_type=jnp.float32))
    current = jax.scipy.linalg.solve_triangular(factor, start_block.T, lower=True).T
    previous = jnp.zeros_like(current)
    upper = factor.T
    basis_list = [current]
    diagonal_list = []
    upper_list = [upper]
    for iteration in range(ITERS):
        work = jnp.dot(covariance.astype(jnp.float32), current.astype(jnp.float32), precision=exact_precision, preferred_element_type=jnp.float32)
        if iteration > 0:
            work = work - jnp.dot(previous.astype(jnp.float32), upper.T.astype(jnp.float32), precision=exact_precision, preferred_element_type=jnp.float32)
        diagonal = jnp.dot(current.T.astype(jnp.float32), work.astype(jnp.float32), precision=exact_precision, preferred_element_type=jnp.float32)
        work = work - jnp.dot(current.astype(jnp.float32), diagonal.astype(jnp.float32), precision=exact_precision, preferred_element_type=jnp.float32)
        factor = lower_factor(jnp.dot(work.T.astype(jnp.float32), work.astype(jnp.float32), precision=exact_precision, preferred_element_type=jnp.float32))
        upper = factor.T
        previous = current
        current = jax.scipy.linalg.solve_triangular(factor, work.T, lower=True).T
        basis_list.append(current)
        diagonal_list.append(diagonal)
        upper_list.append(upper)
    return (covariance, jnp.stack(basis_list), jnp.stack(diagonal_list), jnp.stack(upper_list))
```

```python
import functools
import math

import jax
import jax.numpy as jnp
from jax import lax
from jax.experimental import pallas as pl
from jax.experimental.pallas import tpu as pltpu
from jax.sharding import PartitionSpec as P

L = 48
M = 384
B = 64
ITERS = 6
ROWS = 144
HALF = ROWS // 2
PLANE = 16
LINE = 8
COLS = PLANE * ROWS

exact_precision = lax.Precision.HIGHEST
MESH = pl.DeviceIdType.MESH


def passed_along(block, axis, distance):
    devices = range(lax.axis_size(axis))
    route = [(i - distance, i) for i in devices if i - distance in devices]
    return lax.ppermute(block, axis, route)


def lag_block(local_rows, extended, first_lag, lag_width):
    day_count = local_rows.shape[1]
    span = day_count + lag_width - 1
    segment = extended[:, first_lag : first_lag + span]
    repeated = jnp.tile(segment, (1, lag_width + 1))[:, : lag_width * (span + 1)]
    windows = repeated.reshape(segment.shape[0], lag_width, span + 1)[:, :, :day_count]
    return jnp.einsum(
        "lt,mjt->ljm",
        local_rows,
        windows,
        precision=exact_precision,
        preferred_element_type=jnp.float32,
    )


def lag_products(local_rows, extended):
    lag_width = math.gcd(M, 128)
    parts_list = [
        lag_block(local_rows, extended, first_lag, lag_width)
        for first_lag in range(0, M, lag_width)
    ]
    return jnp.concatenate(parts_list, axis=1)


def split3(x):
    hi = x.astype(jnp.bfloat16)
    rest = x - hi.astype(jnp.float32)
    mid = rest.astype(jnp.bfloat16)
    low = (rest - mid.astype(jnp.float32)).astype(jnp.bfloat16)
    return hi, mid, low


def assemble_kernel(window_ref, hi_ref, mid_ref, low_ref):
    for offset in range(12):
        pieces = [
            window_ref[0, :, L * (11 - offset + 12 * plane) : L * (11 - offset + 12 * plane) + ROWS]
            for plane in range(PLANE)
        ]
        rows = jnp.concatenate(pieces, axis=1)
        hi, mid, low = split3(rows)
        at = slice(L * offset, L * offset + L)
        hi_ref[0, at, :] = hi
        mid_ref[0, at, :] = mid
        low_ref[0, at, :] = low


def assemble(windows):
    width = windows.shape[2]
    shape = jax.ShapeDtypeStruct((2, 12 * L, COLS), jnp.bfloat16)
    spec = pl.BlockSpec((1, 12 * L, COLS), lambda h: (h, 0, 0))
    return pl.pallas_call(
        assemble_kernel,
        grid=(2,),
        out_shape=(shape, shape, shape),
        in_specs=[pl.BlockSpec((1, L, width), lambda h: (h, 0, 0))],
        out_specs=(spec, spec, spec),
        compiler_params=pltpu.CompilerParams(vmem_limit_bytes=60 * 1024 * 1024),
    )(windows)


def exact_dot(left, right, contract):
    return lax.dot_general(
        left,
        right,
        (contract, ((), ())),
        precision=exact_precision,
        preferred_element_type=jnp.float32,
    )


def factor(gram):
    rows = lax.broadcasted_iota(jnp.int32, (B, 2 * B), 0)
    lanes = lax.broadcasted_iota(jnp.int32, (B, 2 * B), 1)
    small_rows = lax.broadcasted_iota(jnp.int32, (B, B), 0)
    small_lanes = lax.broadcasted_iota(jnp.int32, (B, B), 1)
    identity = jnp.where(small_rows == small_lanes, 1.0, 0.0).astype(jnp.float32)
    work = jnp.concatenate([gram, identity], axis=1)
    width = 4
    for first in range(0, B, width):
        columns = [
            jnp.broadcast_to(work[:, first + t : first + t + 1], (B, 2 * B)) for t in range(width)
        ]
        for t in range(width):
            k = first + t
            column = columns[t]
            scale = 1.0 / column[k : k + 1, :]
            weight = jnp.where(rows > k, column * scale, 0.0)
            work = work - weight * work[k : k + 1, :]
            for u in range(t + 1, width):
                columns[u] = columns[u] - weight * column[first + u : first + u + 1, :]
    pivots = jnp.sum(jnp.where(rows == lanes, work, 0.0), axis=1, keepdims=True)
    scaled = work * lax.rsqrt(pivots)
    upper = jnp.where(small_lanes >= small_rows, scaled[:, :B], 0.0)
    inverse = jnp.where(small_lanes <= small_rows, scaled[:, B:], 0.0)
    return upper, inverse


def lanczos_kernel(
    start_ref,
    hi_ref,
    mid_ref,
    low_ref,
    basis_ref,
    diag_ref,
    off_ref,
    work,
    current,
    packed,
    gathered,
    stacked,
    partial,
    landed,
    gram,
    stage1,
    slab,
    stage2,
    total,
    full,
    send_q,
    recv_q,
    send_p,
    recv_p,
    send_1,
    recv_1,
    send_2,
    recv_2,
    send_3,
    recv_3,
):
    tm = lax.axis_index("tm")
    panel = lax.axis_index("panel")
    low_z = tm // PLANE
    plane = tm % PLANE
    line = low_z * 4 + panel

    def plane_peer(step):
        spot_x = (plane // 4 + step // 4) % 4
        spot_y = (plane % 4 + step % 4) % 4
        spot = spot_x * 4 + spot_y
        return spot, (low_z * PLANE + spot, panel)

    def line_peer(step):
        spot_z = (low_z + step // 4) % 2
        spot_p = (panel + step % 4) % 4
        return spot_z * 4 + spot_p, (spot_z * PLANE + plane, spot_p)

    barrier = pltpu.get_barrier_semaphore()
    for step in range(1, PLANE):
        pl.semaphore_signal(barrier, inc=1, device_id=plane_peer(step)[1], device_id_type=MESH)
    for step in range(1, LINE):
        pl.semaphore_signal(barrier, inc=1, device_id=line_peer(step)[1], device_id_type=MESH)
    pl.semaphore_wait(barrier, PLANE + LINE - 2)

    def plane_copy(step, source, target, sends, receives):
        spot, device = plane_peer(step)
        return pltpu.make_async_remote_copy(
            src_ref=source,
            dst_ref=target.at[plane],
            send_sem=sends.at[step],
            recv_sem=receives.at[step],
            device_id=device,
            device_id_type=MESH,
        )

    def line_copy(step, source, target, sends, receives):
        return pltpu.make_async_remote_copy(
            src_ref=source,
            dst_ref=target,
            send_sem=sends.at[step],
            recv_sem=receives.at[step],
            device_id=line_peer(step)[1],
            device_id_type=MESH,
        )

    def gram_total(basis_block, rows_block):
        both = jnp.concatenate([basis_block, rows_block], axis=1)
        gram[...] = exact_dot(both, both, ((0,), (0,))).reshape(LINE, 16, 2 * B)
        firsts = [
            line_copy(step, gram.at[line_peer(step)[0]], stage1.at[line], send_1, recv_1)
            for step in range(1, LINE)
        ]
        for copy in firsts:
            copy.start()
        stage1[line] = gram[line]
        for copy in firsts:
            copy.wait()
        reduced = stage1[0]
        for spot in range(1, LINE):
            reduced = reduced + stage1[spot]
        slab[...] = reduced
        stage2[plane] = reduced
        seconds = [plane_copy(step, slab, stage2, send_2, recv_2) for step in range(1, PLANE)]
        for copy in seconds:
            copy.start()
        for copy in seconds:
            copy.wait()
        reduced = stage2[0]
        for spot in range(1, PLANE):
            reduced = reduced + stage2[spot]
        total[...] = reduced
        full[line] = reduced
        thirds = [line_copy(step, total, full.at[line], send_3, recv_3) for step in range(1, LINE)]
        for copy in thirds:
            copy.start()
        for copy in thirds:
            copy.wait()
        return full[...].reshape(2 * B, 2 * B)

    work[...] = start_ref[...]
    current[...] = jnp.zeros_like(current)

    def one_step(step_at, carry):
        summed = gram_total(current[...], work[...])
        basis_gram = summed[:B, :B]
        diagonal = summed[:B, B:]
        work_gram = summed[B:, B:]
        weighted = exact_dot(basis_gram, diagonal, ((1,), (0,)))
        left = exact_dot(diagonal, 2.0 * diagonal - weighted, ((0,), (0,)))
        upper, inverse = factor(work_gram - left)
        reduced = work[...] - exact_dot(current[...], diagonal, ((1,), (0,)))
        fresh = exact_dot(reduced, inverse, ((1,), (1,)))
        diag_ref[step_at] = diagonal
        off_ref[step_at] = upper
        basis_ref[step_at] = fresh

        @pl.when(step_at < ITERS)
        def _():
            block = jnp.concatenate([fresh[:HALF], fresh[HALF:]], axis=1)
            packed[...] = block
            gathered[plane] = block
            copies = [plane_copy(step, packed, gathered, send_q, recv_q) for step in range(1, PLANE)]
            for copy in copies:
                copy.start()
            back = exact_dot(current[...], upper, ((1,), (1,)))
            current[...] = fresh
            for copy in copies:
                copy.wait()

            def unpack(spot, carry):
                block = gathered[spot]
                block = jnp.concatenate([block[:, :B], block[:, B:]], axis=0)
                hi, mid, low = split3(block)
                at = pl.ds(pl.multiple_of(spot * ROWS, ROWS), ROWS)
                stacked[at, :] = jnp.concatenate([hi, mid, low], axis=1)
                return carry

            lax.fori_loop(0, PLANE, unpack, 0)

            def multiply(h, carry):
                first = jnp.dot(hi_ref[h], stacked[...], preferred_element_type=jnp.float32)
                second = jnp.dot(
                    mid_ref[h], stacked[:, : 2 * B], preferred_element_type=jnp.float32
                )
                third = jnp.dot(low_ref[h], stacked[:, :B], preferred_element_type=jnp.float32)
                low_part = third + second[:, B:] + first[:, 2 * B :]
                product = first[:, :B] + (first[:, B : 2 * B] + second[:, :B] + low_part)
                for spot in range(4):
                    rows = product[spot * ROWS : (spot + 1) * ROWS]
                    partial[h * 4 + spot] = jnp.concatenate([rows[:HALF], rows[HALF:]], axis=1)
                return carry

            lax.fori_loop(0, 2, multiply, 0)
            sums = [
                line_copy(step, partial.at[line_peer(step)[0]], landed.at[line], send_p, recv_p)
                for step in range(1, LINE)
            ]
            for copy in sums:
                copy.start()
            landed[line] = partial[line]
            for copy in sums:
                copy.wait()
            value = landed[0]
            for spot in range(1, LINE):
                value = value + landed[spot]
            work[...] = jnp.concatenate([value[:, :B], value[:, B:]], axis=0) - back

        return carry

    lax.fori_loop(0, ITERS + 1, one_step, 0)


def lanczos(start, hi, mid, low):
    vmem = pl.BlockSpec(memory_space=pltpu.VMEM)
    dma = pltpu.SemaphoreType.DMA
    return pl.pallas_call(
        lanczos_kernel,
        out_shape=(
            jax.ShapeDtypeStruct((ITERS + 1, ROWS, B), jnp.float32),
            jax.ShapeDtypeStruct((ITERS + 1, B, B), jnp.float32),
            jax.ShapeDtypeStruct((ITERS + 1, B, B), jnp.float32),
        ),
        in_specs=[vmem] * 4,
        out_specs=(vmem, vmem, vmem),
        scratch_shapes=[
            pltpu.VMEM((ROWS, B), jnp.float32),
            pltpu.VMEM((ROWS, B), jnp.float32),
            pltpu.VMEM((HALF, 2 * B), jnp.float32),
            pltpu.VMEM((PLANE, HALF, 2 * B), jnp.float32),
            pltpu.VMEM((COLS, 3 * B), jnp.bfloat16),
            pltpu.VMEM((LINE, HALF, 2 * B), jnp.float32),
            pltpu.VMEM((LINE, HALF, 2 * B), jnp.float32),
            pltpu.VMEM((LINE, 16, 2 * B), jnp.float32),
            pltpu.VMEM((LINE, 16, 2 * B), jnp.float32),
            pltpu.VMEM((16, 2 * B), jnp.float32),
            pltpu.VMEM((PLANE, 16, 2 * B), jnp.float32),
            pltpu.VMEM((16, 2 * B), jnp.float32),
            pltpu.VMEM((LINE, 16, 2 * B), jnp.float32),
            dma((PLANE,)),
            dma((PLANE,)),
            dma((LINE,)),
            dma((LINE,)),
            dma((LINE,)),
            dma((LINE,)),
            dma((PLANE,)),
            dma((PLANE,)),
            dma((LINE,)),
            dma((LINE,)),
        ],
        compiler_params=pltpu.CompilerParams(
            collective_id=0, has_side_effects=True, vmem_limit_bytes=60 * 1024 * 1024
        ),
    )(start, hi, mid, low)


def local(series, start_block):
    channels, day_count = series.shape
    tm_size = lax.axis_size("tm")
    panel_size = lax.axis_size("panel")
    total_days = day_count * tm_size
    reach_hops = (M - 1 + day_count - 1) // day_count
    pieces = [series]
    moving = series
    for distance in range(reach_hops):
        moving = passed_along(moving, "tm", -1)
        pieces.append(moving)
    extended = jnp.concatenate(pieces, axis=1)
    summed = lax.psum(lag_products(series, extended), "tm")
    counts = (total_days - jnp.arange(M)).astype(jnp.float32)
    normed = summed / counts[None, :, None]
    two_sided = jnp.concatenate([jnp.transpose(normed, (2, 1, 0))[:, :0:-1, :], normed], axis=1)
    flat = two_sided.reshape(channels, (2 * M - 1) * channels)
    tm = lax.axis_index("tm")
    panel = lax.axis_index("panel")
    block_index = tm * panel_size + panel
    covariance = jnp.concatenate(
        [
            lax.dynamic_slice(
                flat, (0, (M - 1 - 3 * block_index - offset) * channels), (channels, M * channels)
            )
            for offset in range(3)
        ],
        axis=0,
    )
    windows = jnp.stack(
        [
            lax.dynamic_slice(
                flat,
                (0, (372 + (tm // PLANE - h) * 192 - 12 * (tm % PLANE) + 3 * panel) * channels),
                (channels, 194 * channels),
            )
            for h in range(2)
        ]
    )
    hi, mid, low = assemble(windows)
    basis, diag, off = lanczos(start_block, hi, mid, low)
    return covariance, basis, diag[1:], off


def solution(mesh):
    placed = (P(None, "tm"), P(("tm", "panel"), None))
    return jax.shard_map(
        local,
        mesh=mesh,
        in_specs=placed,
        out_specs=(P(("tm", "panel"), None), P(None, ("tm", "panel"), None), P(), P()),
        check_vma=False,
    )
```

```python
import functools

import jax
import jax.numpy as jnp
from jax import lax
from jax.experimental import pallas as pl
from jax.experimental.pallas import tpu as pltpu
from jax.sharding import PartitionSpec as P

L = 48
M = 384
B = 64
ITERS = 6
ROWS = 144
HALF = ROWS // 2
PLANE = 16
LINE = 8
COLS = PLANE * ROWS
LANES = 128
DAYS = 256
SPAN = PLANE * DAYS
LAGS = 12

exact_precision = lax.Precision.HIGHEST
MESH = pl.DeviceIdType.MESH


def split3(x):
    hi = x.astype(jnp.bfloat16)
    rest = x - hi.astype(jnp.float32)
    mid = rest.astype(jnp.bfloat16)
    low = (rest - mid.astype(jnp.float32)).astype(jnp.bfloat16)
    return hi, mid, low


def peers(plane, low_z, panel):
    def plane_peer(step):
        spot_x = (plane // 4 + step // 4) % 4
        spot_y = (plane % 4 + step % 4) % 4
        spot = spot_x * 4 + spot_y
        return spot, (low_z * PLANE + spot, panel)

    return plane_peer


def rolled_window(ref, start, width):
    first = start // LANES
    rest = start % LANES
    lanes = lax.broadcasted_iota(jnp.int32, (L, LANES), 1)
    pieces = [
        pltpu.roll(
            ref[:, pl.ds(pl.multiple_of((first + at) * LANES, LANES), LANES)],
            (LANES - rest) % LANES,
            1,
        )
        for at in range(width // LANES + 1)
    ]
    kept = lanes < LANES - rest
    joined = [jnp.where(kept, pieces[at], pieces[at + 1]) for at in range(width // LANES)]
    return jnp.concatenate(joined, axis=1)


def lag_kernel(
    series_ref,
    out_ref,
    flat,
    shifted,
    own,
    win_hi,
    win_mid,
    win_low,
    mine,
    theirs,
    send_s,
    recv_s,
    send_c,
    recv_c,
    send_f,
    recv_f,
    send_h,
    recv_h,
):
    tm = lax.axis_index("tm")
    panel = lax.axis_index("panel")
    low_z = tm // PLANE
    plane = tm % PLANE
    core = panel % 2
    group = plane * 2 + core
    plane_peer = peers(plane, low_z, panel)
    across = ((1 - low_z) * PLANE + plane, panel)
    beside = (tm, panel + 1 - 2 * core)

    barrier = pltpu.get_barrier_semaphore()
    for step in range(1, PLANE):
        pl.semaphore_signal(barrier, inc=1, device_id=plane_peer(step)[1], device_id_type=MESH)
    pl.semaphore_signal(barrier, inc=1, device_id=across, device_id_type=MESH)
    pl.semaphore_signal(barrier, inc=1, device_id=beside, device_id_type=MESH)
    pl.semaphore_wait(barrier, PLANE + 1)

    def remote(source, target, send, receive, device):
        return pltpu.make_async_remote_copy(
            src_ref=source,
            dst_ref=target,
            send_sem=send,
            recv_sem=receive,
            device_id=device,
            device_id_type=MESH,
        )

    place = pl.ds(pl.multiple_of(plane * DAYS, DAYS), DAYS)
    days = [
        remote(series_ref, flat.at[:, place], send_s.at[step], recv_s.at[step], plane_peer(step)[1])
        for step in range(1, PLANE)
    ]
    for copy in days:
        copy.start()
    flat[:, place] = series_ref[...]
    for copy in days:
        copy.wait()
    halo = remote(
        flat.at[:, : 2 * DAYS], flat.at[:, SPAN : SPAN + 2 * DAYS], send_h.at[0], recv_h.at[0], across
    )
    halo.start()
    hi, mid, low = split3(flat[:, :SPAN])
    own[:L] = hi
    own[L : 2 * L] = mid
    own[2 * L :] = low
    halo.wait()
    beyond = flat[:, SPAN : SPAN + 2 * DAYS]
    flat[:, SPAN : SPAN + 2 * DAYS] = jnp.where(low_z == 1, jnp.zeros_like(beyond), beyond)
    shifted[...] = rolled_window(flat, group * LAGS, SPAN + LANES)
    for lag in range(LAGS):
        hi, mid, low = split3(shifted[:, lag : lag + SPAN])
        at = slice(L * lag, L * lag + L)
        win_hi[at, :] = hi
        win_mid[at, :] = mid
        win_low[at, :] = low

    def product(left, right):
        return lax.dot_general(
            left, right, (((1,), (1,)), ((), ())), preferred_element_type=jnp.float32
        )

    first = product(win_hi[...], own[...])
    second = product(win_mid[...], own[: 2 * L])
    third = product(win_low[...], own[:L])
    low_part = first[:, 2 * L :] + second[:, L:] + third
    sums = first[:, :L] + (first[:, L : 2 * L] + second[:, :L] + low_part)
    mine[...] = jnp.transpose(sums)
    half = remote(mine, theirs, send_h.at[1], recv_h.at[1], across)
    half.start()
    lanes = lax.broadcasted_iota(jnp.int32, (L, LAGS * L), 1)
    lag_at = jnp.zeros_like(lanes)
    for lag in range(1, LAGS):
        lag_at = lag_at + jnp.where(lanes >= lag * L, 1, 0)
    counts = (2 * SPAN - (group * LAGS + lag_at)).astype(jnp.float32)
    half.wait()
    out_ref[group] = (mine[...] + theirs[...]) / counts
    sends = [
        remote(
            out_ref.at[group], out_ref.at[group], send_c.at[step], recv_c.at[step], plane_peer(step)[1]
        )
        for step in range(1, PLANE)
    ]
    for copy in sends:
        copy.start()
    passed = [remote(out_ref.at[group], out_ref.at[group], send_f.at[0], recv_f.at[0], beside)]
    passed[0].start()
    for step in range(1, PLANE):
        sends[step - 1].wait_recv()
        spot_x = (plane // 4 + 4 - step // 4) % 4
        spot_y = (plane % 4 + 4 - step % 4) % 4
        slot = (spot_x * 4 + spot_y) * 2 + core
        copy = remote(out_ref.at[slot], out_ref.at[slot], send_f.at[step], recv_f.at[step], beside)
        copy.start()
        passed.append(copy)
    for copy in sends:
        copy.wait_send()
    for copy in passed:
        copy.wait()


def lag_blocks(series):
    vmem = pl.BlockSpec(memory_space=pltpu.VMEM)
    dma = pltpu.SemaphoreType.DMA
    return pl.pallas_call(
        lag_kernel,
        out_shape=jax.ShapeDtypeStruct((2 * PLANE, L, LAGS * L), jnp.float32),
        in_specs=[vmem],
        out_specs=vmem,
        scratch_shapes=[
            pltpu.VMEM((L, SPAN + 2 * DAYS), jnp.float32),
            pltpu.VMEM((L, SPAN + LANES), jnp.float32),
            pltpu.VMEM((3 * L, SPAN), jnp.bfloat16),
            pltpu.VMEM((LAGS * L, SPAN), jnp.bfloat16),
            pltpu.VMEM((LAGS * L, SPAN), jnp.bfloat16),
            pltpu.VMEM((LAGS * L, SPAN), jnp.bfloat16),
            pltpu.VMEM((L, LAGS * L), jnp.float32),
            pltpu.VMEM((L, LAGS * L), jnp.float32),
            dma((PLANE,)),
            dma((PLANE,)),
            dma((PLANE,)),
            dma((PLANE,)),
            dma((PLANE,)),
            dma((PLANE,)),
            dma((2,)),
            dma((2,)),
        ],
        compiler_params=pltpu.CompilerParams(
            collective_id=1, has_side_effects=True, vmem_limit_bytes=60 * 1024 * 1024
        ),
    )(series)


def assemble_kernel(blocks_ref, cov_ref, hi_ref, mid_ref, low_ref, line):
    tm = lax.axis_index("tm")
    panel = lax.axis_index("panel")
    low_z = tm // PLANE
    plane = tm % PLANE
    step = pl.program_id(0)
    pair = 2 * LAGS * L

    @pl.when(step == 0)
    def _():
        def lay(at, carry):
            both = jnp.concatenate([blocks_ref[2 * at], blocks_ref[2 * at + 1]], axis=1)
            line[:, pl.ds(pl.multiple_of(M * L + at * pair, LANES), pair)] = both
            after = blocks_ref[jnp.minimum(2 * at + 2, 2 * PLANE - 1)][:, :LANES]
            turned = jnp.transpose(jnp.concatenate([both, after], axis=1))
            reversed_blocks = [
                turned[L * lag : L * lag + L, :] for lag in range(2 * LAGS, 0, -1)
            ]
            line[:, pl.ds(pl.multiple_of((PLANE - 1 - at) * pair, LANES), pair)] = jnp.concatenate(
                reversed_blocks, axis=1
            )
            return carry

        lax.fori_loop(0, PLANE, lay, 0)

    own_lag = 3 * (tm * 4 + panel)
    for offset in range(3):
        start = L * (M - own_lag - offset) + step * COLS
        cov_ref[L * offset : L * offset + L, :] = rolled_window(line, start, COLS)
    h = step // 4
    spot = step % 4
    base = L * (372 + (low_z - h) * 192 - 12 * plane + 3 * panel + 12 - 3 * spot - 2)
    window = rolled_window(line, base, 71 * LANES)
    for offset in range(3):
        pieces = [
            window[:, L * (2 - offset + 12 * at) : L * (2 - offset + 12 * at) + ROWS]
            for at in range(PLANE)
        ]
        hi, mid, low = split3(jnp.concatenate(pieces, axis=1))
        at = slice(L * offset, L * offset + L)
        hi_ref[0, at, :] = hi
        mid_ref[0, at, :] = mid
        low_ref[0, at, :] = low


def assemble(blocks):
    shape = jax.ShapeDtypeStruct((LINE, ROWS, COLS), jnp.bfloat16)
    spec = pl.BlockSpec((1, ROWS, COLS), lambda h: (h, 0, 0))
    return pl.pallas_call(
        assemble_kernel,
        grid=(LINE,),
        out_shape=(jax.ShapeDtypeStruct((ROWS, M * L), jnp.float32), shape, shape, shape),
        in_specs=[pl.BlockSpec((2 * PLANE, L, LAGS * L), lambda h: (0, 0, 0))],
        out_specs=(pl.BlockSpec((ROWS, COLS), lambda h: (0, h)), spec, spec, spec),
        scratch_shapes=[pltpu.VMEM((L, 2 * M * L + 2 * LANES), jnp.float32)],
        compiler_params=pltpu.CompilerParams(vmem_limit_bytes=60 * 1024 * 1024),
    )(blocks)


def exact_dot(left, right, contract):
    return lax.dot_general(
        left,
        right,
        (contract, ((), ())),
        precision=exact_precision,
        preferred_element_type=jnp.float32,
    )


def factor(gram):
    rows = lax.broadcasted_iota(jnp.int32, (B, 2 * B), 0)
    lanes = lax.broadcasted_iota(jnp.int32, (B, 2 * B), 1)
    small_rows = lax.broadcasted_iota(jnp.int32, (B, B), 0)
    small_lanes = lax.broadcasted_iota(jnp.int32, (B, B), 1)
    identity = jnp.where(small_rows == small_lanes, 1.0, 0.0).astype(jnp.float32)
    work = jnp.concatenate([gram, identity], axis=1)
    width = 4
    for first in range(0, B, width):
        columns = [
            jnp.broadcast_to(work[:, first + t : first + t + 1], (B, 2 * B)) for t in range(width)
        ]
        for t in range(width):
            k = first + t
            column = columns[t]
            scale = 1.0 / column[k : k + 1, :]
            weight = jnp.where(rows > k, column * scale, 0.0)
            work = work - weight * work[k : k + 1, :]
            for u in range(t + 1, width):
                columns[u] = columns[u] - weight * column[first + u : first + u + 1, :]
    pivots = jnp.sum(jnp.where(rows == lanes, work, 0.0), axis=1, keepdims=True)
    scaled = work * lax.rsqrt(pivots)
    upper = jnp.where(small_lanes >= small_rows, scaled[:, :B], 0.0)
    inverse = jnp.where(small_lanes <= small_rows, scaled[:, B:], 0.0)
    return upper, inverse


def lanczos_kernel(
    start_ref,
    hi_ref,
    mid_ref,
    low_ref,
    basis_ref,
    diag_ref,
    off_ref,
    work,
    current,
    packed,
    gathered,
    stacked,
    partial,
    landed,
    gram,
    stage1,
    slab,
    stage2,
    total,
    full,
    send_q,
    recv_q,
    send_p,
    recv_p,
    send_1,
    recv_1,
    send_2,
    recv_2,
    send_3,
    recv_3,
):
    tm = lax.axis_index("tm")
    panel = lax.axis_index("panel")
    low_z = tm // PLANE
    plane = tm % PLANE
    line = low_z * 4 + panel

    def plane_peer(step):
        spot_x = (plane // 4 + step // 4) % 4
        spot_y = (plane % 4 + step % 4) % 4
        spot = spot_x * 4 + spot_y
        return spot, (low_z * PLANE + spot, panel)

    def line_peer(step):
        spot_z = (low_z + step // 4) % 2
        spot_p = (panel + step % 4) % 4
        return spot_z * 4 + spot_p, (spot_z * PLANE + plane, spot_p)

    barrier = pltpu.get_barrier_semaphore()
    for step in range(1, PLANE):
        pl.semaphore_signal(barrier, inc=1, device_id=plane_peer(step)[1], device_id_type=MESH)
    for step in range(1, LINE):
        pl.semaphore_signal(barrier, inc=1, device_id=line_peer(step)[1], device_id_type=MESH)
    pl.semaphore_wait(barrier, PLANE + LINE - 2)

    def plane_copy(step, source, target, sends, receives):
        spot, device = plane_peer(step)
        return pltpu.make_async_remote_copy(
            src_ref=source,
            dst_ref=target.at[plane],
            send_sem=sends.at[step],
            recv_sem=receives.at[step],
            device_id=device,
            device_id_type=MESH,
        )

    def line_copy(step, source, target, sends, receives):
        return pltpu.make_async_remote_copy(
            src_ref=source,
            dst_ref=target,
            send_sem=sends.at[step],
            recv_sem=receives.at[step],
            device_id=line_peer(step)[1],
            device_id_type=MESH,
        )

    def gram_total(basis_block, rows_block):
        both = jnp.concatenate([basis_block, rows_block], axis=1)
        gram[...] = exact_dot(both, both, ((0,), (0,))).reshape(LINE, 16, 2 * B)
        firsts = [
            line_copy(step, gram.at[line_peer(step)[0]], stage1.at[line], send_1, recv_1)
            for step in range(1, LINE)
        ]
        for copy in firsts:
            copy.start()
        stage1[line] = gram[line]
        for copy in firsts:
            copy.wait()
        reduced = stage1[0]
        for spot in range(1, LINE):
            reduced = reduced + stage1[spot]
        slab[...] = reduced
        stage2[plane] = reduced
        seconds = [plane_copy(step, slab, stage2, send_2, recv_2) for step in range(1, PLANE)]
        for copy in seconds:
            copy.start()
        for copy in seconds:
            copy.wait()
        reduced = stage2[0]
        for spot in range(1, PLANE):
            reduced = reduced + stage2[spot]
        total[...] = reduced
        full[line] = reduced
        thirds = [line_copy(step, total, full.at[line], send_3, recv_3) for step in range(1, LINE)]
        for copy in thirds:
            copy.start()
        for copy in thirds:
            copy.wait()
        return full[...].reshape(2 * B, 2 * B)

    work[...] = start_ref[...]
    current[...] = jnp.zeros_like(current)

    def one_step(step_at, carry):
        summed = gram_total(current[...], work[...])
        basis_gram = summed[:B, :B]
        diagonal = summed[:B, B:]
        work_gram = summed[B:, B:]
        weighted = exact_dot(basis_gram, diagonal, ((1,), (0,)))
        left = exact_dot(diagonal, 2.0 * diagonal - weighted, ((0,), (0,)))
        upper, inverse = factor(work_gram - left)
        reduced = work[...] - exact_dot(current[...], diagonal, ((1,), (0,)))
        fresh = exact_dot(reduced, inverse, ((1,), (1,)))
        diag_ref[step_at] = diagonal
        off_ref[step_at] = upper
        basis_ref[step_at] = fresh

        @pl.when(step_at < ITERS)
        def _():
            block = jnp.concatenate([fresh[:HALF], fresh[HALF:]], axis=1)
            packed[...] = block
            gathered[plane] = block
            copies = [plane_copy(step, packed, gathered, send_q, recv_q) for step in range(1, PLANE)]
            for copy in copies:
                copy.start()
            back = exact_dot(current[...], upper, ((1,), (1,)))
            current[...] = fresh
            for copy in copies:
                copy.wait()

            def unpack(spot, carry):
                block = gathered[spot]
                block = jnp.concatenate([block[:, :B], block[:, B:]], axis=0)
                hi, mid, low = split3(block)
                at = pl.ds(pl.multiple_of(spot * ROWS, ROWS), ROWS)
                stacked[at, :] = jnp.concatenate([hi, mid, low], axis=1)
                return carry

            lax.fori_loop(0, PLANE, unpack, 0)

            def multiply(h, carry):
                first = jnp.dot(hi_ref[h], stacked[...], preferred_element_type=jnp.float32)
                second = jnp.dot(
                    mid_ref[h], stacked[:, : 2 * B], preferred_element_type=jnp.float32
                )
                third = jnp.dot(low_ref[h], stacked[:, :B], preferred_element_type=jnp.float32)
                low_part = third + second[:, B:] + first[:, 2 * B :]
                product = first[:, :B] + (first[:, B : 2 * B] + second[:, :B] + low_part)
                for spot in range(4):
                    rows = product[spot * ROWS : (spot + 1) * ROWS]
                    partial[h * 4 + spot] = jnp.concatenate([rows[:HALF], rows[HALF:]], axis=1)
                return carry

            lax.fori_loop(0, 2, multiply, 0)
            sums = [
                line_copy(step, partial.at[line_peer(step)[0]], landed.at[line], send_p, recv_p)
                for step in range(1, LINE)
            ]
            for copy in sums:
                copy.start()
            landed[line] = partial[line]
            for copy in sums:
                copy.wait()
            value = landed[0]
            for spot in range(1, LINE):
                value = value + landed[spot]
            work[...] = jnp.concatenate([value[:, :B], value[:, B:]], axis=0) - back

        return carry

    lax.fori_loop(0, ITERS + 1, one_step, 0)


def lanczos(start, hi, mid, low):
    vmem = pl.BlockSpec(memory_space=pltpu.VMEM)
    dma = pltpu.SemaphoreType.DMA
    return pl.pallas_call(
        lanczos_kernel,
        out_shape=(
            jax.ShapeDtypeStruct((ITERS + 1, ROWS, B), jnp.float32),
            jax.ShapeDtypeStruct((ITERS + 1, B, B), jnp.float32),
            jax.ShapeDtypeStruct((ITERS + 1, B, B), jnp.float32),
        ),
        in_specs=[vmem] * 4,
        out_specs=(vmem, vmem, vmem),
        scratch_shapes=[
            pltpu.VMEM((ROWS, B), jnp.float32),
            pltpu.VMEM((ROWS, B), jnp.float32),
            pltpu.VMEM((HALF, 2 * B), jnp.float32),
            pltpu.VMEM((PLANE, HALF, 2 * B), jnp.float32),
            pltpu.VMEM((COLS, 3 * B), jnp.bfloat16),
            pltpu.VMEM((LINE, HALF, 2 * B), jnp.float32),
            pltpu.VMEM((LINE, HALF, 2 * B), jnp.float32),
            pltpu.VMEM((LINE, 16, 2 * B), jnp.float32),
            pltpu.VMEM((LINE, 16, 2 * B), jnp.float32),
            pltpu.VMEM((16, 2 * B), jnp.float32),
            pltpu.VMEM((PLANE, 16, 2 * B), jnp.float32),
            pltpu.VMEM((16, 2 * B), jnp.float32),
            pltpu.VMEM((LINE, 16, 2 * B), jnp.float32),
            dma((PLANE,)),
            dma((PLANE,)),
            dma((LINE,)),
            dma((LINE,)),
            dma((LINE,)),
            dma((LINE,)),
            dma((PLANE,)),
            dma((PLANE,)),
            dma((LINE,)),
            dma((LINE,)),
        ],
        compiler_params=pltpu.CompilerParams(
            collective_id=0, has_side_effects=True, vmem_limit_bytes=60 * 1024 * 1024
        ),
    )(start, hi, mid, low)


def local(series, start_block):
    covariance, hi, mid, low = assemble(lag_blocks(series))
    shape = (2, 12 * L, COLS)
    basis, diag, off = lanczos(start_block, hi.reshape(shape), mid.reshape(shape), low.reshape(shape))
    return covariance, basis, diag[1:], off


def solution(mesh):
    placed = (P(None, "tm"), P(("tm", "panel"), None))
    return jax.shard_map(
        local,
        mesh=mesh,
        in_specs=placed,
        out_specs=(P(("tm", "panel"), None), P(None, ("tm", "panel"), None), P(), P()),
        check_vma=False,
    )
```

```python
import functools

import jax
import jax.numpy as jnp
from jax import lax
from jax.experimental import pallas as pl
from jax.experimental.pallas import tpu as pltpu
from jax.sharding import PartitionSpec as P

L = 48
M = 384
B = 64
ITERS = 6
ROWS = 144
HALF = ROWS // 2
PLANE = 16
LINE = 8
COLS = PLANE * ROWS
LANES = 128
DAYS = 256
SPAN = PLANE * DAYS
LAGS = 12

exact_precision = lax.Precision.HIGHEST
MESH = pl.DeviceIdType.MESH


def split3(x):
    hi = x.astype(jnp.bfloat16)
    rest = x - hi.astype(jnp.float32)
    mid = rest.astype(jnp.bfloat16)
    low = (rest - mid.astype(jnp.float32)).astype(jnp.bfloat16)
    return hi, mid, low


def peers(plane, low_z, panel):
    def plane_peer(step):
        spot_x = (plane // 4 + step // 4) % 4
        spot_y = (plane % 4 + step % 4) % 4
        spot = spot_x * 4 + spot_y
        return spot, (low_z * PLANE + spot, panel)

    return plane_peer


def rolled_window(ref, start, width):
    first = start // LANES
    rest = start % LANES
    lanes = lax.broadcasted_iota(jnp.int32, (L, LANES), 1)
    pieces = [
        pltpu.roll(
            ref[:, pl.ds(pl.multiple_of((first + at) * LANES, LANES), LANES)],
            (LANES - rest) % LANES,
            1,
        )
        for at in range(width // LANES + 1)
    ]
    kept = lanes < LANES - rest
    joined = [jnp.where(kept, pieces[at], pieces[at + 1]) for at in range(width // LANES)]
    return jnp.concatenate(joined, axis=1)


def lag_kernel(
    series_ref,
    out_ref,
    flat,
    shifted,
    own,
    win_hi,
    win_mid,
    win_low,
    mine,
    theirs,
    send_s,
    recv_s,
    send_c,
    recv_c,
    send_f,
    recv_f,
    send_h,
    recv_h,
):
    tm = lax.axis_index("tm")
    panel = lax.axis_index("panel")
    low_z = tm // PLANE
    plane = tm % PLANE
    core = panel % 2
    group = plane * 2 + core
    plane_peer = peers(plane, low_z, panel)
    across = ((1 - low_z) * PLANE + plane, panel)
    beside = (tm, panel + 1 - 2 * core)

    barrier = pltpu.get_barrier_semaphore()
    for step in range(1, PLANE):
        pl.semaphore_signal(barrier, inc=1, device_id=plane_peer(step)[1], device_id_type=MESH)
    pl.semaphore_signal(barrier, inc=1, device_id=across, device_id_type=MESH)
    pl.semaphore_signal(barrier, inc=1, device_id=beside, device_id_type=MESH)
    pl.semaphore_wait(barrier, PLANE + 1)

    def remote(source, target, send, receive, device):
        return pltpu.make_async_remote_copy(
            src_ref=source,
            dst_ref=target,
            send_sem=send,
            recv_sem=receive,
            device_id=device,
            device_id_type=MESH,
        )

    place = pl.ds(pl.multiple_of(plane * DAYS, DAYS), DAYS)
    days = [
        remote(series_ref, flat.at[:, place], send_s.at[step], recv_s.at[step], plane_peer(step)[1])
        for step in range(1, PLANE)
    ]
    for copy in days:
        copy.start()
    flat[:, place] = series_ref[...]
    for copy in days:
        copy.wait()
    halo = remote(
        flat.at[:, : 2 * DAYS], flat.at[:, SPAN : SPAN + 2 * DAYS], send_h.at[0], recv_h.at[0], across
    )
    halo.start()
    hi, mid, low = split3(flat[:, :SPAN])
    own[:L] = hi
    own[L : 2 * L] = mid
    own[2 * L :] = low
    halo.wait()
    beyond = flat[:, SPAN : SPAN + 2 * DAYS]
    flat[:, SPAN : SPAN + 2 * DAYS] = jnp.where(low_z == 1, jnp.zeros_like(beyond), beyond)
    shifted[...] = rolled_window(flat, group * LAGS, SPAN + LANES)
    for lag in range(LAGS):
        hi, mid, low = split3(shifted[:, lag : lag + SPAN])
        at = slice(L * lag, L * lag + L)
        win_hi[at, :] = hi
        win_mid[at, :] = mid
        win_low[at, :] = low

    def product(left, right):
        return lax.dot_general(
            left, right, (((1,), (1,)), ((), ())), preferred_element_type=jnp.float32
        )

    first = product(win_hi[...], own[...])
    second = product(win_mid[...], own[: 2 * L])
    third = product(win_low[...], own[:L])
    low_part = first[:, 2 * L :] + second[:, L:] + third
    sums = first[:, :L] + (first[:, L : 2 * L] + second[:, :L] + low_part)
    mine[...] = jnp.transpose(sums)
    half = remote(mine, theirs, send_h.at[1], recv_h.at[1], across)
    half.start()
    lanes = lax.broadcasted_iota(jnp.int32, (L, LAGS * L), 1)
    lag_at = jnp.zeros_like(lanes)
    for lag in range(1, LAGS):
        lag_at = lag_at + jnp.where(lanes >= lag * L, 1, 0)
    counts = (2 * SPAN - (group * LAGS + lag_at)).astype(jnp.float32)
    half.wait()
    out_ref[group] = (mine[...] + theirs[...]) / counts
    sends = [
        remote(
            out_ref.at[group], out_ref.at[group], send_c.at[step], recv_c.at[step], plane_peer(step)[1]
        )
        for step in range(1, PLANE)
    ]
    for copy in sends:
        copy.start()
    passed = [remote(out_ref.at[group], out_ref.at[group], send_f.at[0], recv_f.at[0], beside)]
    passed[0].start()
    for step in range(1, PLANE):
        sends[step - 1].wait_recv()
        spot_x = (plane // 4 + 4 - step // 4) % 4
        spot_y = (plane % 4 + 4 - step % 4) % 4
        slot = (spot_x * 4 + spot_y) * 2 + core
        copy = remote(out_ref.at[slot], out_ref.at[slot], send_f.at[step], recv_f.at[step], beside)
        copy.start()
        passed.append(copy)
    for copy in sends:
        copy.wait_send()
    for copy in passed:
        copy.wait()


def lag_blocks(series):
    vmem = pl.BlockSpec(memory_space=pltpu.VMEM)
    dma = pltpu.SemaphoreType.DMA
    return pl.pallas_call(
        lag_kernel,
        out_shape=jax.ShapeDtypeStruct((2 * PLANE, L, LAGS * L), jnp.float32),
        in_specs=[vmem],
        out_specs=vmem,
        scratch_shapes=[
            pltpu.VMEM((L, SPAN + 2 * DAYS), jnp.float32),
            pltpu.VMEM((L, SPAN + LANES), jnp.float32),
            pltpu.VMEM((3 * L, SPAN), jnp.bfloat16),
            pltpu.VMEM((LAGS * L, SPAN), jnp.bfloat16),
            pltpu.VMEM((LAGS * L, SPAN), jnp.bfloat16),
            pltpu.VMEM((LAGS * L, SPAN), jnp.bfloat16),
            pltpu.VMEM((L, LAGS * L), jnp.float32),
            pltpu.VMEM((L, LAGS * L), jnp.float32),
            dma((PLANE,)),
            dma((PLANE,)),
            dma((PLANE,)),
            dma((PLANE,)),
            dma((PLANE,)),
            dma((PLANE,)),
            dma((2,)),
            dma((2,)),
        ],
        compiler_params=pltpu.CompilerParams(
            collective_id=1, has_side_effects=True, vmem_limit_bytes=60 * 1024 * 1024
        ),
    )(series)


def assemble_kernel(blocks_ref, cov_ref, hi_ref, mid_ref, low_ref, line):
    tm = lax.axis_index("tm")
    panel = lax.axis_index("panel")
    low_z = tm // PLANE
    plane = tm % PLANE
    step = pl.program_id(0)
    pair = 2 * LAGS * L

    @pl.when(step == 0)
    def _():
        def lay(at, carry):
            both = jnp.concatenate([blocks_ref[2 * at], blocks_ref[2 * at + 1]], axis=1)
            line[:, pl.ds(pl.multiple_of(M * L + at * pair, LANES), pair)] = both
            after = blocks_ref[jnp.minimum(2 * at + 2, 2 * PLANE - 1)][:, :LANES]
            turned = jnp.transpose(jnp.concatenate([both, after], axis=1))
            reversed_blocks = [
                turned[L * lag : L * lag + L, :] for lag in range(2 * LAGS, 0, -1)
            ]
            line[:, pl.ds(pl.multiple_of((PLANE - 1 - at) * pair, LANES), pair)] = jnp.concatenate(
                reversed_blocks, axis=1
            )
            return carry

        lax.fori_loop(0, PLANE, lay, 0)

    own_lag = 3 * (tm * 4 + panel)
    for offset in range(3):
        start = L * (M - own_lag - offset) + step * COLS
        cov_ref[L * offset : L * offset + L, :] = rolled_window(line, start, COLS)
    h = step // 4
    spot = step % 4
    base = L * (372 + (low_z - h) * 192 - 12 * plane + 3 * panel + 12 - 3 * spot - 2)
    window = rolled_window(line, base, 71 * LANES)
    for offset in range(3):
        pieces = [
            window[:, L * (2 - offset + 12 * at) : L * (2 - offset + 12 * at) + ROWS]
            for at in range(PLANE)
        ]
        hi, mid, low = split3(jnp.concatenate(pieces, axis=1))
        at = slice(L * offset, L * offset + L)
        hi_ref[0, at, :] = hi
        mid_ref[0, at, :] = mid
        low_ref[0, at, :] = low


def assemble(blocks):
    shape = jax.ShapeDtypeStruct((LINE, ROWS, COLS), jnp.bfloat16)
    spec = pl.BlockSpec((1, ROWS, COLS), lambda h: (h, 0, 0))
    return pl.pallas_call(
        assemble_kernel,
        grid=(LINE,),
        out_shape=(jax.ShapeDtypeStruct((ROWS, M * L), jnp.float32), shape, shape, shape),
        in_specs=[pl.BlockSpec((2 * PLANE, L, LAGS * L), lambda h: (0, 0, 0))],
        out_specs=(pl.BlockSpec((ROWS, COLS), lambda h: (0, h)), spec, spec, spec),
        scratch_shapes=[pltpu.VMEM((L, 2 * M * L + 2 * LANES), jnp.float32)],
        compiler_params=pltpu.CompilerParams(vmem_limit_bytes=60 * 1024 * 1024),
    )(blocks)


def exact_dot(left, right, contract):
    return lax.dot_general(
        left,
        right,
        (contract, ((), ())),
        precision=exact_precision,
        preferred_element_type=jnp.float32,
    )


def factor(gram):
    rows = lax.broadcasted_iota(jnp.int32, (B, 2 * B), 0)
    lanes = lax.broadcasted_iota(jnp.int32, (B, 2 * B), 1)
    small_rows = lax.broadcasted_iota(jnp.int32, (B, B), 0)
    small_lanes = lax.broadcasted_iota(jnp.int32, (B, B), 1)
    identity = jnp.where(small_rows == small_lanes, 1.0, 0.0).astype(jnp.float32)
    work = jnp.concatenate([gram, identity], axis=1)
    width = 4
    for first in range(0, B, width):
        columns = [
            jnp.broadcast_to(work[:, first + t : first + t + 1], (B, 2 * B)) for t in range(width)
        ]
        for t in range(width):
            k = first + t
            column = columns[t]
            scale = 1.0 / column[k : k + 1, :]
            weight = jnp.where(rows > k, column * scale, 0.0)
            work = work - weight * work[k : k + 1, :]
            for u in range(t + 1, width):
                columns[u] = columns[u] - weight * column[first + u : first + u + 1, :]
    pivots = jnp.sum(jnp.where(rows == lanes, work, 0.0), axis=1, keepdims=True)
    scaled = work * lax.rsqrt(pivots)
    upper = jnp.where(small_lanes >= small_rows, scaled[:, :B], 0.0)
    inverse = jnp.where(small_lanes <= small_rows, scaled[:, B:], 0.0)
    return upper, inverse


def hops(step):
    return (0, 1, 2, 1)[step // 4] + (0, 1, 2, 1)[step % 4]


FAR_FIRST = sorted(range(1, PLANE), key=lambda step: -hops(step))


def pack(block):
    return jnp.concatenate([block[:HALF], block[HALF:]], axis=1)


def unpack(block):
    return jnp.concatenate([block[:, :B], block[:, B:]], axis=0)


def lanczos_kernel(
    start_ref,
    hi_ref,
    mid_ref,
    low_ref,
    basis_ref,
    diag_ref,
    off_ref,
    tile_hi,
    tile_mid,
    tile_low,
    work,
    current,
    applied,
    packed,
    gathered,
    stacked,
    partial,
    landed,
    gram,
    stage1,
    slab,
    stage2,
    total,
    full,
    tile_sem,
    send_q,
    recv_q,
    send_p,
    recv_p,
    send_1,
    recv_1,
    send_2,
    recv_2,
    send_3,
    recv_3,
):
    tm = lax.axis_index("tm")
    panel = lax.axis_index("panel")
    low_z = tm // PLANE
    plane = tm % PLANE
    line = low_z * 4 + panel
    tiles = [
        pltpu.make_async_copy(source, target, tile_sem.at[at])
        for at, (source, target) in enumerate(
            ((hi_ref, tile_hi), (mid_ref, tile_mid), (low_ref, tile_low))
        )
    ]
    for copy in tiles:
        copy.start()

    plane_peer = peers(plane, low_z, panel)

    def line_peer(step):
        spot_z = (low_z + step // 4) % 2
        spot_p = (panel + step % 4) % 4
        return spot_z * 4 + spot_p, (spot_z * PLANE + plane, spot_p)

    barrier = pltpu.get_barrier_semaphore()
    for step in range(1, PLANE):
        pl.semaphore_signal(barrier, inc=1, device_id=plane_peer(step)[1], device_id_type=MESH)
    for step in range(1, LINE):
        pl.semaphore_signal(barrier, inc=1, device_id=line_peer(step)[1], device_id_type=MESH)
    pl.semaphore_wait(barrier, PLANE + LINE - 2)

    def remote(source, target, send, receive, device):
        return pltpu.make_async_remote_copy(
            src_ref=source,
            dst_ref=target,
            send_sem=send,
            recv_sem=receive,
            device_id=device,
            device_id_type=MESH,
        )

    work[...] = start_ref[...]
    current[...] = jnp.zeros_like(current)
    applied[...] = jnp.zeros_like(applied)

    def one_step(step_at, last):
        slot = step_at % 2
        before = current[...]
        rows_block = work[...]
        blocks = [
            remote(
                packed,
                gathered.at[slot, plane],
                send_q.at[step],
                recv_q.at[slot, step],
                plane_peer(step)[1],
            )
            for step in FAR_FIRST
            if not last
        ]
        if not last:
            packed[...] = pack(rows_block)
            for copy in blocks:
                copy.start()

        both = jnp.concatenate([before, rows_block], axis=1)
        gram[...] = exact_dot(both, both, ((0,), (0,))).reshape(LINE, 16, 2 * B)
        firsts = [
            remote(
                gram.at[line_peer(step)[0]],
                stage1.at[line],
                send_1.at[step],
                recv_1.at[step],
                line_peer(step)[1],
            )
            for step in range(1, LINE)
        ]
        for copy in firsts:
            copy.start()
        stage1[line] = gram[line]

        def lay(spot, block):
            hi, mid, low = split3(unpack(block))
            at = pl.ds(pl.multiple_of(spot * ROWS, ROWS), ROWS)
            stacked[at, :] = jnp.concatenate([hi, mid, low], axis=1)

        if not last:
            lay(plane, packed[...])
        for copy in firsts:
            copy.wait()
        reduced = stage1[0]
        for spot in range(1, LINE):
            reduced = reduced + stage1[spot]
        slab[...] = reduced
        stage2[slot, plane] = reduced
        seconds = [
            remote(
                slab,
                stage2.at[slot, plane],
                send_2.at[step],
                recv_2.at[slot, step],
                plane_peer(step)[1],
            )
            for step in FAR_FIRST
        ]
        for copy in seconds:
            copy.start()

        sums = [
            remote(
                partial.at[line_peer(step)[0]],
                landed.at[slot, line],
                send_p.at[step],
                recv_p.at[slot, step],
                line_peer(step)[1],
            )
            for step in range(1, LINE)
            if not last
        ]

        def multiply(h, carry):
            first = jnp.dot(tile_hi[h], stacked[...], preferred_element_type=jnp.float32)
            second = jnp.dot(
                tile_mid[h], stacked[:, : 2 * B], preferred_element_type=jnp.float32
            )
            third = jnp.dot(tile_low[h], stacked[:, :B], preferred_element_type=jnp.float32)
            low_part = third + second[:, B:] + first[:, 2 * B :]
            product = first[:, :B] + (first[:, B : 2 * B] + second[:, :B] + low_part)
            for spot in range(4):
                rows = product[spot * ROWS : (spot + 1) * ROWS]
                partial[h * 4 + spot] = pack(rows)
            return carry

        if not last:
            for copy, step in zip(blocks, FAR_FIRST):
                copy.wait()
                spot_x = (plane // 4 + 4 - step // 4) % 4
                spot_y = (plane % 4 + 4 - step % 4) % 4
                spot = spot_x * 4 + spot_y
                lay(spot, gathered[slot, spot])

            @pl.when(step_at == 0)
            def _():
                for copy in tiles:
                    copy.wait()

            lax.fori_loop(0, 2, multiply, 0)
            for copy in sums:
                copy.start()
            landed[slot, line] = partial[line]

        for copy in seconds:
            copy.wait()
        reduced = stage2[slot, 0]
        for spot in range(1, PLANE):
            reduced = reduced + stage2[slot, spot]
        total[...] = reduced
        full[line] = reduced
        thirds = [
            remote(total, full.at[line], send_3.at[step], recv_3.at[step], line_peer(step)[1])
            for step in range(1, LINE)
        ]
        for copy in thirds:
            copy.start()
        for copy in thirds:
            copy.wait()
        summed = full[...].reshape(2 * B, 2 * B)
        basis_gram = summed[:B, :B]
        diagonal = summed[:B, B:]
        work_gram = summed[B:, B:]
        weighted = exact_dot(basis_gram, diagonal, ((1,), (0,)))
        left = exact_dot(diagonal, 2.0 * diagonal - weighted, ((0,), (0,)))
        upper, inverse = factor(work_gram - left)
        diag_ref[jnp.maximum(step_at - 1, 0)] = diagonal
        off_ref[step_at] = upper
        if last:
            reduced = rows_block - exact_dot(before, diagonal, ((1,), (0,)))
            basis_ref[step_at] = exact_dot(reduced, inverse, ((1,), (1,)))
            return
        for copy in sums:
            copy.wait()
        value = landed[slot, 0]
        for spot in range(1, LINE):
            value = value + landed[slot, spot]
        old = jnp.concatenate([before, applied[...]], axis=0)
        new = jnp.concatenate([rows_block, unpack(value)], axis=0)
        reduced = new - exact_dot(old, diagonal, ((1,), (0,)))
        fresh = exact_dot(reduced, inverse, ((1,), (1,)))
        basis_ref[step_at] = fresh[:ROWS]
        current[...] = fresh[:ROWS]
        applied[...] = fresh[ROWS:]
        work[...] = fresh[ROWS:] - exact_dot(before, upper, ((1,), (1,)))

    def body(step_at, carry):
        one_step(step_at, False)
        return carry

    lax.fori_loop(0, ITERS, body, 0)
    one_step(ITERS, True)


def lanczos(start, hi, mid, low):
    vmem = pl.BlockSpec(memory_space=pltpu.VMEM)
    away = pl.BlockSpec(memory_space=pl.ANY)
    dma = pltpu.SemaphoreType.DMA
    tile = pltpu.VMEM((2, 4 * ROWS, COLS), jnp.bfloat16)
    return pl.pallas_call(
        lanczos_kernel,
        out_shape=(
            jax.ShapeDtypeStruct((ITERS + 1, ROWS, B), jnp.float32),
            jax.ShapeDtypeStruct((ITERS, B, B), jnp.float32),
            jax.ShapeDtypeStruct((ITERS + 1, B, B), jnp.float32),
        ),
        in_specs=[vmem, away, away, away],
        out_specs=(vmem, vmem, vmem),
        scratch_shapes=[
            tile,
            tile,
            tile,
            pltpu.VMEM((ROWS, B), jnp.float32),
            pltpu.VMEM((ROWS, B), jnp.float32),
            pltpu.VMEM((ROWS, B), jnp.float32),
            pltpu.VMEM((HALF, 2 * B), jnp.float32),
            pltpu.VMEM((2, PLANE, HALF, 2 * B), jnp.float32),
            pltpu.VMEM((COLS, 3 * B), jnp.bfloat16),
            pltpu.VMEM((LINE, HALF, 2 * B), jnp.float32),
            pltpu.VMEM((2, LINE, HALF, 2 * B), jnp.float32),
            pltpu.VMEM((LINE, 16, 2 * B), jnp.float32),
            pltpu.VMEM((LINE, 16, 2 * B), jnp.float32),
            pltpu.VMEM((16, 2 * B), jnp.float32),
            pltpu.VMEM((2, PLANE, 16, 2 * B), jnp.float32),
            pltpu.VMEM((16, 2 * B), jnp.float32),
            pltpu.VMEM((LINE, 16, 2 * B), jnp.float32),
            dma((3,)),
            dma((PLANE,)),
            dma((2, PLANE)),
            dma((LINE,)),
            dma((2, LINE)),
            dma((LINE,)),
            dma((LINE,)),
            dma((PLANE,)),
            dma((2, PLANE)),
            dma((LINE,)),
            dma((LINE,)),
        ],
        compiler_params=pltpu.CompilerParams(
            collective_id=0, has_side_effects=True, vmem_limit_bytes=60 * 1024 * 1024
        ),
    )(start, hi, mid, low)


def local(series, start_block):
    covariance, hi, mid, low = assemble(lag_blocks(series))
    shape = (2, 12 * L, COLS)
    basis, diag, off = lanczos(start_block, hi.reshape(shape), mid.reshape(shape), low.reshape(shape))
    return covariance, basis, diag, off


def solution(mesh):
    placed = (P(None, "tm"), P(("tm", "panel"), None))
    return jax.shard_map(
        local,
        mesh=mesh,
        in_specs=placed,
        out_specs=(P(("tm", "panel"), None), P(None, ("tm", "panel"), None), P(), P()),
        check_vma=False,
    )
```

```python
import functools

import jax
import jax.numpy as jnp
from jax import lax
from jax.experimental import pallas as pl
from jax.experimental.pallas import tpu as pltpu
from jax.sharding import PartitionSpec as P

L = 48
M = 384
B = 64
ITERS = 6
ROWS = 144
HALF = ROWS // 2
PLANE = 16
LINE = 8
COLS = PLANE * ROWS
HALF_COLS = COLS // 2
LANES = 128
DAYS = 256
SPAN = PLANE * DAYS
LAGS = 12

exact_precision = lax.Precision.HIGHEST
MESH = pl.DeviceIdType.MESH


def split3(x):
    hi = x.astype(jnp.bfloat16)
    rest = x - hi.astype(jnp.float32)
    mid = rest.astype(jnp.bfloat16)
    low = (rest - mid.astype(jnp.float32)).astype(jnp.bfloat16)
    return hi, mid, low


def peers(plane, low_z, panel):
    def plane_peer(step):
        spot_x = (plane // 4 + step // 4) % 4
        spot_y = (plane % 4 + step % 4) % 4
        spot = spot_x * 4 + spot_y
        return spot, (low_z * PLANE + spot, panel)

    return plane_peer


def rolled_window(ref, start, width):
    first = start // LANES
    rest = start % LANES
    lanes = lax.broadcasted_iota(jnp.int32, (L, LANES), 1)
    pieces = [
        pltpu.roll(
            ref[:, pl.ds(pl.multiple_of((first + at) * LANES, LANES), LANES)],
            (LANES - rest) % LANES,
            1,
        )
        for at in range(width // LANES + 1)
    ]
    kept = lanes < LANES - rest
    joined = [jnp.where(kept, pieces[at], pieces[at + 1]) for at in range(width // LANES)]
    return jnp.concatenate(joined, axis=1)


def lag_kernel(
    series_ref,
    out_ref,
    flat,
    shifted,
    own,
    win_hi,
    win_mid,
    win_low,
    mine,
    theirs,
    send_s,
    recv_s,
    send_c,
    recv_c,
    send_f,
    recv_f,
    send_h,
    recv_h,
):
    tm = lax.axis_index("tm")
    panel = lax.axis_index("panel")
    low_z = tm // PLANE
    plane = tm % PLANE
    core = panel % 2
    group = plane * 2 + core
    plane_peer = peers(plane, low_z, panel)
    across = ((1 - low_z) * PLANE + plane, panel)
    beside = (tm, panel + 1 - 2 * core)

    barrier = pltpu.get_barrier_semaphore()
    for step in range(1, PLANE):
        pl.semaphore_signal(barrier, inc=1, device_id=plane_peer(step)[1], device_id_type=MESH)
    pl.semaphore_signal(barrier, inc=1, device_id=across, device_id_type=MESH)
    pl.semaphore_signal(barrier, inc=1, device_id=beside, device_id_type=MESH)
    pl.semaphore_wait(barrier, PLANE + 1)

    def remote(source, target, send, receive, device):
        return pltpu.make_async_remote_copy(
            src_ref=source,
            dst_ref=target,
            send_sem=send,
            recv_sem=receive,
            device_id=device,
            device_id_type=MESH,
        )

    place = pl.ds(pl.multiple_of(plane * DAYS, DAYS), DAYS)
    days = [
        remote(series_ref, flat.at[:, place], send_s.at[step], recv_s.at[step], plane_peer(step)[1])
        for step in range(1, PLANE)
    ]
    for copy in days:
        copy.start()
    flat[:, place] = series_ref[...]
    for copy in days:
        copy.wait()
    halo = remote(
        flat.at[:, : 2 * DAYS], flat.at[:, SPAN : SPAN + 2 * DAYS], send_h.at[0], recv_h.at[0], across
    )
    halo.start()
    hi, mid, low = split3(flat[:, :SPAN])
    own[:L] = hi
    own[L : 2 * L] = mid
    own[2 * L :] = low
    halo.wait()
    beyond = flat[:, SPAN : SPAN + 2 * DAYS]
    flat[:, SPAN : SPAN + 2 * DAYS] = jnp.where(low_z == 1, jnp.zeros_like(beyond), beyond)
    shifted[...] = rolled_window(flat, group * LAGS, SPAN + LANES)
    for lag in range(LAGS):
        hi, mid, low = split3(shifted[:, lag : lag + SPAN])
        at = slice(L * lag, L * lag + L)
        win_hi[at, :] = hi
        win_mid[at, :] = mid
        win_low[at, :] = low

    def product(left, right):
        return lax.dot_general(
            left, right, (((1,), (1,)), ((), ())), preferred_element_type=jnp.float32
        )

    first = product(win_hi[...], own[...])
    second = product(win_mid[...], own[: 2 * L])
    third = product(win_low[...], own[:L])
    low_part = first[:, 2 * L :] + second[:, L:] + third
    sums = first[:, :L] + (first[:, L : 2 * L] + second[:, :L] + low_part)
    mine[...] = jnp.transpose(sums)
    half = remote(mine, theirs, send_h.at[1], recv_h.at[1], across)
    half.start()
    lanes = lax.broadcasted_iota(jnp.int32, (L, LAGS * L), 1)
    lag_at = jnp.zeros_like(lanes)
    for lag in range(1, LAGS):
        lag_at = lag_at + jnp.where(lanes >= lag * L, 1, 0)
    counts = (2 * SPAN - (group * LAGS + lag_at)).astype(jnp.float32)
    half.wait()
    out_ref[group] = (mine[...] + theirs[...]) / counts
    sends = [
        remote(
            out_ref.at[group], out_ref.at[group], send_c.at[step], recv_c.at[step], plane_peer(step)[1]
        )
        for step in range(1, PLANE)
    ]
    for copy in sends:
        copy.start()
    passed = [remote(out_ref.at[group], out_ref.at[group], send_f.at[0], recv_f.at[0], beside)]
    passed[0].start()
    for step in range(1, PLANE):
        sends[step - 1].wait_recv()
        spot_x = (plane // 4 + 4 - step // 4) % 4
        spot_y = (plane % 4 + 4 - step % 4) % 4
        slot = (spot_x * 4 + spot_y) * 2 + core
        copy = remote(out_ref.at[slot], out_ref.at[slot], send_f.at[step], recv_f.at[step], beside)
        copy.start()
        passed.append(copy)
    for copy in sends:
        copy.wait_send()
    for copy in passed:
        copy.wait()


def lag_blocks(series):
    vmem = pl.BlockSpec(memory_space=pltpu.VMEM)
    dma = pltpu.SemaphoreType.DMA
    return pl.pallas_call(
        lag_kernel,
        out_shape=jax.ShapeDtypeStruct((2 * PLANE, L, LAGS * L), jnp.float32),
        in_specs=[vmem],
        out_specs=vmem,
        scratch_shapes=[
            pltpu.VMEM((L, SPAN + 2 * DAYS), jnp.float32),
            pltpu.VMEM((L, SPAN + LANES), jnp.float32),
            pltpu.VMEM((3 * L, SPAN), jnp.bfloat16),
            pltpu.VMEM((LAGS * L, SPAN), jnp.bfloat16),
            pltpu.VMEM((LAGS * L, SPAN), jnp.bfloat16),
            pltpu.VMEM((LAGS * L, SPAN), jnp.bfloat16),
            pltpu.VMEM((L, LAGS * L), jnp.float32),
            pltpu.VMEM((L, LAGS * L), jnp.float32),
            dma((PLANE,)),
            dma((PLANE,)),
            dma((PLANE,)),
            dma((PLANE,)),
            dma((PLANE,)),
            dma((PLANE,)),
            dma((2,)),
            dma((2,)),
        ],
        compiler_params=pltpu.CompilerParams(
            collective_id=1, has_side_effects=True, vmem_limit_bytes=60 * 1024 * 1024
        ),
    )(series)


def assemble_kernel(blocks_ref, cov_ref, hi_ref, mid_ref, low_ref, line):
    tm = lax.axis_index("tm")
    panel = lax.axis_index("panel")
    low_z = tm // PLANE
    plane = tm % PLANE
    step = pl.program_id(0)
    pair = 2 * LAGS * L

    @pl.when(step == 0)
    def _():
        def lay(at, carry):
            both = jnp.concatenate([blocks_ref[2 * at], blocks_ref[2 * at + 1]], axis=1)
            line[:, pl.ds(pl.multiple_of(M * L + at * pair, LANES), pair)] = both
            after = blocks_ref[jnp.minimum(2 * at + 2, 2 * PLANE - 1)][:, :LANES]
            turned = jnp.transpose(jnp.concatenate([both, after], axis=1))
            reversed_blocks = [
                turned[L * lag : L * lag + L, :] for lag in range(2 * LAGS, 0, -1)
            ]
            line[:, pl.ds(pl.multiple_of((PLANE - 1 - at) * pair, LANES), pair)] = jnp.concatenate(
                reversed_blocks, axis=1
            )
            return carry

        lax.fori_loop(0, PLANE, lay, 0)

    own_lag = 3 * (tm * 4 + panel)
    for offset in range(3):
        start = L * (M - own_lag - offset) + step * COLS
        cov_ref[L * offset : L * offset + L, :] = rolled_window(line, start, COLS)
    h = step // 4
    spot = step % 4
    base = L * (372 + (low_z - h) * 192 - 12 * plane + 3 * panel + 12 - 3 * spot - 2)
    window = rolled_window(line, base, 71 * LANES)
    for offset in range(3):
        pieces = [
            window[:, L * (2 - offset + 12 * at) : L * (2 - offset + 12 * at) + ROWS]
            for at in range(PLANE)
        ]
        hi, mid, low = split3(jnp.concatenate(pieces, axis=1))
        at = slice(L * offset, L * offset + L)
        hi_ref[0, at, :] = hi
        mid_ref[0, at, :] = mid
        low_ref[0, at, :] = low


def assemble(blocks):
    shape = jax.ShapeDtypeStruct((LINE, ROWS, COLS), jnp.bfloat16)
    spec = pl.BlockSpec((1, ROWS, COLS), lambda h: (h, 0, 0))
    return pl.pallas_call(
        assemble_kernel,
        grid=(LINE,),
        out_shape=(jax.ShapeDtypeStruct((ROWS, M * L), jnp.float32), shape, shape, shape),
        in_specs=[pl.BlockSpec((2 * PLANE, L, LAGS * L), lambda h: (0, 0, 0))],
        out_specs=(pl.BlockSpec((ROWS, COLS), lambda h: (0, h)), spec, spec, spec),
        scratch_shapes=[pltpu.VMEM((L, 2 * M * L + 2 * LANES), jnp.float32)],
        compiler_params=pltpu.CompilerParams(vmem_limit_bytes=60 * 1024 * 1024),
    )(blocks)


def exact_dot(left, right, contract):
    return lax.dot_general(
        left,
        right,
        (contract, ((), ())),
        precision=exact_precision,
        preferred_element_type=jnp.float32,
    )


def factor(gram):
    rows = lax.broadcasted_iota(jnp.int32, (B, 2 * B), 0)
    lanes = lax.broadcasted_iota(jnp.int32, (B, 2 * B), 1)
    small_rows = lax.broadcasted_iota(jnp.int32, (B, B), 0)
    small_lanes = lax.broadcasted_iota(jnp.int32, (B, B), 1)
    identity = jnp.where(small_rows == small_lanes, 1.0, 0.0).astype(jnp.float32)
    work = jnp.concatenate([gram, identity], axis=1)
    width = 4
    for first in range(0, B, width):
        columns = [
            jnp.broadcast_to(work[:, first + t : first + t + 1], (B, 2 * B)) for t in range(width)
        ]
        for t in range(width):
            k = first + t
            column = columns[t]
            scale = 1.0 / column[k : k + 1, :]
            weight = jnp.where(rows > k, column * scale, 0.0)
            work = work - weight * work[k : k + 1, :]
            for u in range(t + 1, width):
                columns[u] = columns[u] - weight * column[first + u : first + u + 1, :]
    pivots = jnp.sum(jnp.where(rows == lanes, work, 0.0), axis=1, keepdims=True)
    scaled = work * lax.rsqrt(pivots)
    upper = jnp.where(small_lanes >= small_rows, scaled[:, :B], 0.0)
    inverse = jnp.where(small_lanes <= small_rows, scaled[:, B:], 0.0)
    return upper, inverse


PAIR_FIRST = [(0, y) for y in (2, 1, 3)] + [(1, y) for y in (2, 1, 3, 0)]
PAIR_LAST = [(2, y) for y in (2, 1, 3, 0)] + [(3, y) for y in (2, 1, 3, 0)]
FAR_FIRST = [10, 6, 14, 9, 11, 2, 8, 5, 7, 13, 15, 1, 3, 4, 12]


def pack(block):
    return jnp.concatenate([block[:HALF], block[HALF:]], axis=1)


def unpack(block):
    return jnp.concatenate([block[:, :B], block[:, B:]], axis=0)


def lanczos_kernel(
    start_ref,
    hi_ref,
    mid_ref,
    low_ref,
    basis_ref,
    diag_ref,
    off_ref,
    tile_hi,
    tile_mid,
    tile_low,
    work,
    current,
    applied,
    packed,
    gathered,
    stacked,
    accumulated,
    partial,
    landed,
    gram,
    stage1,
    slab,
    stage2,
    total,
    full,
    tile_sem,
    send_q,
    recv_q,
    send_p,
    recv_p,
    send_1,
    recv_1,
    send_2,
    recv_2,
    send_3,
    recv_3,
):
    tm = lax.axis_index("tm")
    panel = lax.axis_index("panel")
    low_z = tm // PLANE
    plane = tm % PLANE
    line = low_z * 4 + panel
    tiles = [
        pltpu.make_async_copy(source, target, tile_sem.at[at])
        for at, (source, target) in enumerate(
            ((hi_ref, tile_hi), (mid_ref, tile_mid), (low_ref, tile_low))
        )
    ]
    for copy in tiles:
        copy.start()

    plane_peer = peers(plane, low_z, panel)

    def line_peer(step):
        spot_z = (low_z + step // 4) % 2
        spot_p = (panel + step % 4) % 4
        return spot_z * 4 + spot_p, (spot_z * PLANE + plane, spot_p)

    pair_at = plane // 8
    odd_x = (plane // 4) % 2

    def x_at(turn):
        side = (pair_at + turn // 2) % 2
        return side * 2 + (odd_x + turn) % 2

    barrier = pltpu.get_barrier_semaphore()
    for step in range(1, PLANE):
        pl.semaphore_signal(barrier, inc=1, device_id=plane_peer(step)[1], device_id_type=MESH)
    for step in range(1, LINE):
        pl.semaphore_signal(barrier, inc=1, device_id=line_peer(step)[1], device_id_type=MESH)
    pl.semaphore_wait(barrier, PLANE + LINE - 2)

    def remote(source, target, send, receive, device):
        return pltpu.make_async_remote_copy(
            src_ref=source,
            dst_ref=target,
            send_sem=send,
            recv_sem=receive,
            device_id=device,
            device_id_type=MESH,
        )

    work[...] = start_ref[...]
    current[...] = jnp.zeros_like(current)
    applied[...] = jnp.zeros_like(applied)

    def one_step(step_at, last):
        slot = step_at % 2
        before = current[...]
        rows_block = work[...]

        def block_copies(places, first):
            found = []
            for at, (turn, y) in enumerate(places):
                to_x = x_at(turn)
                to_y = (plane % 4 + y) % 4
                from_y = (plane % 4 + 4 - y) % 4
                to_spot = to_x * 4 + to_y
                copy = remote(
                    packed,
                    gathered.at[slot, plane],
                    send_q.at[first + at],
                    recv_q.at[slot, first + at],
                    (low_z * PLANE + to_spot, panel),
                )
                found.append((copy, x_at(turn) * 4 + from_y))
            return found

        near = [] if last else block_copies(PAIR_FIRST, 0)
        far = [] if last else block_copies(PAIR_LAST, len(PAIR_FIRST))
        if not last:
            packed[...] = pack(rows_block)
            for copy, _ in near + far:
                copy.start()

        both = jnp.concatenate([before, rows_block], axis=1)
        gram[...] = exact_dot(both, both, ((0,), (0,))).reshape(LINE, 16, 2 * B)
        firsts = [
            remote(
                gram.at[line_peer(step)[0]],
                stage1.at[line],
                send_1.at[step],
                recv_1.at[step],
                line_peer(step)[1],
            )
            for step in range(1, LINE)
        ]
        for copy in firsts:
            copy.start()
        stage1[line] = gram[line]

        def lay(spot, block):
            hi, mid, low = split3(unpack(block))
            at = pl.ds(pl.multiple_of(spot * ROWS, ROWS), ROWS)
            stacked[at, :] = jnp.concatenate([hi, mid, low], axis=1)

        if not last:
            lay(plane, packed[...])
        for copy in firsts:
            copy.wait()
        reduced = stage1[0]
        for spot in range(1, LINE):
            reduced = reduced + stage1[spot]
        slab[...] = reduced
        stage2[slot, plane] = reduced
        seconds = [
            remote(
                slab,
                stage2.at[slot, plane],
                send_2.at[step],
                recv_2.at[slot, step],
                plane_peer(step)[1],
            )
            for step in FAR_FIRST
        ]
        for copy in seconds:
            copy.start()

        sums = [
            remote(
                partial.at[line_peer(step)[0]],
                landed.at[slot, line],
                send_p.at[step],
                recv_p.at[slot, step],
                line_peer(step)[1],
            )
            for step in range(1, LINE)
            if not last
        ]

        def multiply(h, half):
            lanes = pl.ds(pl.multiple_of(half * HALF_COLS, HALF_COLS), HALF_COLS)
            first = jnp.dot(tile_hi[h, :, lanes], stacked[lanes, :], preferred_element_type=jnp.float32)
            second = jnp.dot(
                tile_mid[h, :, lanes], stacked[lanes, : 2 * B], preferred_element_type=jnp.float32
            )
            third = jnp.dot(
                tile_low[h, :, lanes], stacked[lanes, :B], preferred_element_type=jnp.float32
            )
            low_part = third + second[:, B:] + first[:, 2 * B :]
            return first[:, :B] + (first[:, B : 2 * B] + second[:, :B] + low_part)

        def send_sums(h):
            for at, copy in enumerate(sums):
                @pl.when((low_z + (at + 1) // 4) % 2 == h)
                def _():
                    copy.start()

            @pl.when(low_z == h)
            def _():
                landed[slot, line] = partial[line]

        def finish(h):
            product = accumulated[h] + multiply(h, other)
            for spot in range(4):
                rows = product[spot * ROWS : (spot + 1) * ROWS]
                partial[h * 4 + spot] = pack(rows)
            send_sums(h)

        other = 1 - pair_at
        if not last:
            for copy, spot in near:
                copy.wait()
                lay(spot, gathered[slot, spot])

            @pl.when(step_at == 0)
            def _():
                for copy in tiles:
                    copy.wait()

            def begin(h, carry):
                accumulated[h] = multiply(h, pair_at)
                return carry

            lax.fori_loop(0, 2, begin, 0)
            for copy, spot in far:
                copy.wait()
                lay(spot, gathered[slot, spot])
            finish(0)

        for copy in seconds:
            copy.wait()
        reduced = stage2[slot, 0]
        for spot in range(1, PLANE):
            reduced = reduced + stage2[slot, spot]
        total[...] = reduced
        full[line] = reduced
        thirds = [
            remote(total, full.at[line], send_3.at[step], recv_3.at[step], line_peer(step)[1])
            for step in range(1, LINE)
        ]
        for copy in thirds:
            copy.start()
        if not last:
            finish(1)
        for copy in thirds:
            copy.wait()
        summed = full[...].reshape(2 * B, 2 * B)
        basis_gram = summed[:B, :B]
        diagonal = summed[:B, B:]
        work_gram = summed[B:, B:]
        weighted = exact_dot(basis_gram, diagonal, ((1,), (0,)))
        left = exact_dot(diagonal, 2.0 * diagonal - weighted, ((0,), (0,)))
        upper, inverse = factor(work_gram - left)
        diag_ref[jnp.maximum(step_at - 1, 0)] = diagonal
        off_ref[step_at] = upper
        if last:
            reduced = rows_block - exact_dot(before, diagonal, ((1,), (0,)))
            basis_ref[step_at] = exact_dot(reduced, inverse, ((1,), (1,)))
            return
        for copy in sums:
            copy.wait()
        value = landed[slot, 0]
        for spot in range(1, LINE):
            value = value + landed[slot, spot]
        old = jnp.concatenate([before, applied[...]], axis=0)
        new = jnp.concatenate([rows_block, unpack(value)], axis=0)
        reduced = new - exact_dot(old, diagonal, ((1,), (0,)))
        fresh = exact_dot(reduced, inverse, ((1,), (1,)))
        basis_ref[step_at] = fresh[:ROWS]
        current[...] = fresh[:ROWS]
        applied[...] = fresh[ROWS:]
        work[...] = fresh[ROWS:] - exact_dot(before, upper, ((1,), (1,)))

    def body(step_at, carry):
        one_step(step_at, False)
        return carry

    lax.fori_loop(0, ITERS, body, 0)
    one_step(ITERS, True)


def lanczos(start, hi, mid, low):
    vmem = pl.BlockSpec(memory_space=pltpu.VMEM)
    away = pl.BlockSpec(memory_space=pl.ANY)
    dma = pltpu.SemaphoreType.DMA
    tile = pltpu.VMEM((2, 4 * ROWS, COLS), jnp.bfloat16)
    return pl.pallas_call(
        lanczos_kernel,
        out_shape=(
            jax.ShapeDtypeStruct((ITERS + 1, ROWS, B), jnp.float32),
            jax.ShapeDtypeStruct((ITERS, B, B), jnp.float32),
            jax.ShapeDtypeStruct((ITERS + 1, B, B), jnp.float32),
        ),
        in_specs=[vmem, away, away, away],
        out_specs=(vmem, vmem, vmem),
        scratch_shapes=[
            tile,
            tile,
            tile,
            pltpu.VMEM((ROWS, B), jnp.float32),
            pltpu.VMEM((ROWS, B), jnp.float32),
            pltpu.VMEM((ROWS, B), jnp.float32),
            pltpu.VMEM((HALF, 2 * B), jnp.float32),
            pltpu.VMEM((2, PLANE, HALF, 2 * B), jnp.float32),
            pltpu.VMEM((COLS, 3 * B), jnp.bfloat16),
            pltpu.VMEM((2, 4 * ROWS, B), jnp.float32),
            pltpu.VMEM((LINE, HALF, 2 * B), jnp.float32),
            pltpu.VMEM((2, LINE, HALF, 2 * B), jnp.float32),
            pltpu.VMEM((LINE, 16, 2 * B), jnp.float32),
            pltpu.VMEM((LINE, 16, 2 * B), jnp.float32),
            pltpu.VMEM((16, 2 * B), jnp.float32),
            pltpu.VMEM((2, PLANE, 16, 2 * B), jnp.float32),
            pltpu.VMEM((16, 2 * B), jnp.float32),
            pltpu.VMEM((LINE, 16, 2 * B), jnp.float32),
            dma((3,)),
            dma((PLANE,)),
            dma((2, PLANE)),
            dma((LINE,)),
            dma((2, LINE)),
            dma((LINE,)),
            dma((LINE,)),
            dma((PLANE,)),
            dma((2, PLANE)),
            dma((LINE,)),
            dma((LINE,)),
        ],
        compiler_params=pltpu.CompilerParams(
            collective_id=0, has_side_effects=True, vmem_limit_bytes=60 * 1024 * 1024
        ),
    )(start, hi, mid, low)


def local(series, start_block):
    covariance, hi, mid, low = assemble(lag_blocks(series))
    shape = (2, 12 * L, COLS)
    basis, diag, off = lanczos(start_block, hi.reshape(shape), mid.reshape(shape), low.reshape(shape))
    return covariance, basis, diag, off


def solution(mesh):
    placed = (P(None, "tm"), P(("tm", "panel"), None))
    return jax.shard_map(
        local,
        mesh=mesh,
        in_specs=placed,
        out_specs=(P(("tm", "panel"), None), P(None, ("tm", "panel"), None), P(), P()),
        check_vma=False,
    )
```

```python
import functools

import jax
import jax.numpy as jnp
from jax import lax
from jax.experimental import pallas as pl
from jax.experimental.pallas import tpu as pltpu
from jax.sharding import PartitionSpec as P

L = 48
M = 384
B = 64
ITERS = 6
ROWS = 144
HALF = ROWS // 2
PLANE = 16
LINE = 8
COLS = PLANE * ROWS
HALF_COLS = COLS // 2
LANES = 128
DAYS = 256
SPAN = PLANE * DAYS
LAGS = 12

exact_precision = lax.Precision.HIGHEST
MESH = pl.DeviceIdType.MESH


def split3(x):
    hi = x.astype(jnp.bfloat16)
    rest = x - hi.astype(jnp.float32)
    mid = rest.astype(jnp.bfloat16)
    low = (rest - mid.astype(jnp.float32)).astype(jnp.bfloat16)
    return hi, mid, low


def peers(plane, low_z, panel):
    def plane_peer(step):
        spot_x = (plane // 4 + step // 4) % 4
        spot_y = (plane % 4 + step % 4) % 4
        spot = spot_x * 4 + spot_y
        return spot, (low_z * PLANE + spot, panel)

    return plane_peer


def rolled_window(ref, start, width):
    first = start // LANES
    rest = start % LANES
    lanes = lax.broadcasted_iota(jnp.int32, (L, LANES), 1)
    pieces = [
        pltpu.roll(
            ref[:, pl.ds(pl.multiple_of((first + at) * LANES, LANES), LANES)],
            (LANES - rest) % LANES,
            1,
        )
        for at in range(width // LANES + 1)
    ]
    kept = lanes < LANES - rest
    joined = [jnp.where(kept, pieces[at], pieces[at + 1]) for at in range(width // LANES)]
    return jnp.concatenate(joined, axis=1)


def lag_kernel(
    series_ref,
    line,
    blocks,
    flat,
    shifted,
    own,
    win_hi,
    win_mid,
    win_low,
    mine,
    theirs,
    send_s,
    recv_s,
    send_d,
    recv_d,
    send_c,
    recv_c,
    send_f,
    recv_f,
    send_h,
    recv_h,
):
    tm = lax.axis_index("tm")
    panel = lax.axis_index("panel")
    low_z = tm // PLANE
    plane = tm % PLANE
    core = panel % 2
    group = plane * 2 + core
    plane_peer = peers(plane, low_z, panel)
    across = ((1 - low_z) * PLANE + plane, panel)
    beside = (tm, panel + 1 - 2 * core)

    barrier = pltpu.get_barrier_semaphore()
    for step in range(1, PLANE):
        pl.semaphore_signal(barrier, inc=1, device_id=plane_peer(step)[1], device_id_type=MESH)
    pl.semaphore_signal(barrier, inc=1, device_id=across, device_id_type=MESH)
    pl.semaphore_signal(barrier, inc=1, device_id=beside, device_id_type=MESH)
    pl.semaphore_wait(barrier, PLANE + 1)

    def remote(source, target, send, receive, device):
        return pltpu.make_async_remote_copy(
            src_ref=source,
            dst_ref=target,
            send_sem=send,
            recv_sem=receive,
            device_id=device,
            device_id_type=MESH,
        )

    x = plane // 4
    y = plane % 4
    share = L // 2

    def spot_at(turn_x, turn_y):
        return ((x + turn_x) % 4) * 4 + (y + turn_y) % 4

    def chip_at(spot):
        return (low_z * PLANE + spot, panel)

    turns = [(p, q) for p in (2, 1, 3, 0) for q in (2, 1, 3, 0) if p or q]
    rows = pl.ds(pl.multiple_of(core * share, share), share)

    def place(spot):
        return pl.ds(pl.multiple_of(spot * DAYS, DAYS), DAYS)

    flat[:, place(plane)] = series_ref[...]
    days = [
        remote(
            series_ref.at[rows],
            flat.at[rows, place(plane)],
            send_s.at[at],
            recv_s.at[at],
            chip_at(spot_at(*turn)),
        )
        for at, turn in enumerate(turns)
    ]
    for copy in days:
        copy.start()
    shared = []
    for at, turn in enumerate(turns):
        days[at].wait_recv()
        held = flat.at[rows, place(spot_at(-turn[0] + 4, -turn[1] + 4))]
        copy = remote(held, held, send_d.at[at], recv_d.at[at], beside)
        copy.start()
        shared.append(copy)
    for copy in days:
        copy.wait_send()
    for copy in shared:
        copy.wait()
    halo = remote(
        flat.at[:, : 2 * DAYS], flat.at[:, SPAN : SPAN + 2 * DAYS], send_h.at[0], recv_h.at[0], across
    )
    halo.start()
    hi, mid, low = split3(flat[:, :SPAN])
    own[:L] = hi
    own[L : 2 * L] = mid
    own[2 * L :] = low
    halo.wait()
    beyond = flat[:, SPAN : SPAN + 2 * DAYS]
    flat[:, SPAN : SPAN + 2 * DAYS] = jnp.where(low_z == 1, jnp.zeros_like(beyond), beyond)
    shifted[...] = rolled_window(flat, group * LAGS, SPAN + LANES)
    for lag in range(LAGS):
        hi, mid, low = split3(shifted[:, lag : lag + SPAN])
        at = slice(L * lag, L * lag + L)
        win_hi[at, :] = hi
        win_mid[at, :] = mid
        win_low[at, :] = low

    def product(left, right):
        return lax.dot_general(
            left, right, (((1,), (1,)), ((), ())), preferred_element_type=jnp.float32
        )

    first = product(win_hi[...], own[...])
    second = product(win_mid[...], own[: 2 * L])
    third = product(win_low[...], own[:L])
    low_part = first[:, 2 * L :] + second[:, L:] + third
    sums = first[:, :L] + (first[:, L : 2 * L] + second[:, :L] + low_part)
    mine[...] = jnp.transpose(sums)
    half = remote(mine, theirs, send_h.at[1], recv_h.at[1], across)
    half.start()
    lanes = lax.broadcasted_iota(jnp.int32, (L, LAGS * L), 1)
    lag_at = jnp.zeros_like(lanes)
    for lag in range(1, LAGS):
        lag_at = lag_at + jnp.where(lanes >= lag * L, 1, 0)
    counts = (2 * SPAN - (group * LAGS + lag_at)).astype(jnp.float32)
    half.wait()
    blocks[group] = (mine[...] + theirs[...]) / counts

    def held(spot, color):
        return blocks.at[spot * 2 + core, pl.ds(color * share, share)]

    started = []

    def forward(origin_x, origin_y, color, along, to_turn):
        to_x, to_y = (to_turn, 0) if along == 0 else (0, to_turn)
        source = held(spot_at(4 - origin_x, 4 - origin_y), color)
        key = (origin_x + to_x) % 4 * 4 + (origin_y + to_y) % 4
        copy = remote(
            source,
            source,
            send_c.at[color, key],
            recv_c.at[color, key],
            chip_at(spot_at(to_x, to_y)),
        )
        copy.start()
        started.append(copy)

    def landed(origin_x, origin_y, color):
        key = origin_x * 4 + origin_y
        part = held(spot_at(4 - origin_x, 4 - origin_y), color)
        remote(part, part, send_c.at[color, key], recv_c.at[color, key], chip_at(plane)).wait_recv()
        give(origin_x, origin_y, color)

    def give(origin_x, origin_y, color):
        key = origin_x * 4 + origin_y
        part = held(spot_at(4 - origin_x, 4 - origin_y), color)
        copy = remote(part, part, send_f.at[color, key], recv_f.at[color, key], beside)
        copy.start()
        passed[color, key] = copy

    passed = {}
    for turn in (2, 1, 3):
        forward(0, 0, 0, 0, turn)
        forward(0, 0, 1, 1, turn)
    for turn in (2, 1, 3):
        forward(0, 0, 0, 1, turn)
        forward(0, 0, 1, 0, turn)
    for color in range(2):
        give(0, 0, color)

    lanes = lax.broadcasted_iota(jnp.int32, (L, LANES), 1)
    pair = 2 * LAGS * L

    def lay(at):
        both = jnp.concatenate([blocks[2 * at], blocks[2 * at + 1]], axis=1)
        line[:, pl.ds(pl.multiple_of(M * L + at * pair, LANES), pair)] = both
        turned = jnp.transpose(both)
        parts = [turned[L * lag : L * lag + L, :] for lag in range(2 * LAGS - 1, -1, -1)]
        filler = jnp.zeros((L, L), jnp.float32)
        tail = jnp.zeros((L, LANES - L), jnp.float32)
        wide = jnp.concatenate([filler] + parts + [tail], axis=1)
        start = (PLANE - 1 - at) * pair
        front = pl.ds(pl.multiple_of(start, LANES), LANES)
        inner = pl.ds(pl.multiple_of(start + LANES, LANES), pair - LANES)
        back = pl.ds(pl.multiple_of(start + pair, LANES), LANES)
        line[:, front] = jnp.where(lanes < L, line[:, front], wide[:, :LANES])
        line[:, inner] = wide[:, LANES:pair]

        @pl.when(at > 0)
        def _():
            line[:, back] = jnp.where(lanes < L, wide[:, pair:], line[:, back])

    def settle(origin_x, origin_y):
        key = origin_x * 4 + origin_y
        for color in range(2):
            passed[color, key].wait()
        lay(spot_at(4 - origin_x, 4 - origin_y))

    first_wave = (1, 3, 2)
    for turn in first_wave:
        landed(turn, 0, 0)
        for to_turn in (2, 1, 3):
            forward(turn, 0, 0, 1, to_turn)
        landed(0, turn, 1)
        for to_turn in (2, 1, 3):
            forward(0, turn, 1, 0, to_turn)
    settle(0, 0)
    for turn in first_wave:
        landed(0, turn, 0)
        landed(turn, 0, 1)
        settle(0, turn)
        settle(turn, 0)
    for turn_x in first_wave:
        for turn_y in first_wave:
            landed(turn_x, turn_y, 0)
            landed(turn_x, turn_y, 1)
            settle(turn_x, turn_y)
    for copy in started:
        copy.wait_send()


def lag_blocks(series):
    vmem = pl.BlockSpec(memory_space=pltpu.VMEM)
    dma = pltpu.SemaphoreType.DMA
    return pl.pallas_call(
        lag_kernel,
        out_shape=jax.ShapeDtypeStruct((L, 2 * M * L + 2 * LANES), jnp.float32),
        in_specs=[vmem],
        out_specs=vmem,
        scratch_shapes=[
            pltpu.VMEM((2 * PLANE, L, LAGS * L), jnp.float32),
            pltpu.VMEM((L, SPAN + 2 * DAYS), jnp.float32),
            pltpu.VMEM((L, SPAN + LANES), jnp.float32),
            pltpu.VMEM((3 * L, SPAN), jnp.bfloat16),
            pltpu.VMEM((LAGS * L, SPAN), jnp.bfloat16),
            pltpu.VMEM((LAGS * L, SPAN), jnp.bfloat16),
            pltpu.VMEM((LAGS * L, SPAN), jnp.bfloat16),
            pltpu.VMEM((L, LAGS * L), jnp.float32),
            pltpu.VMEM((L, LAGS * L), jnp.float32),
            dma((PLANE,)),
            dma((PLANE,)),
            dma((PLANE,)),
            dma((PLANE,)),
            dma((2, PLANE)),
            dma((2, PLANE)),
            dma((2, PLANE)),
            dma((2, PLANE)),
            dma((2,)),
            dma((2,)),
        ],
        compiler_params=pltpu.CompilerParams(
            collective_id=1, has_side_effects=True, vmem_limit_bytes=60 * 1024 * 1024
        ),
    )(series)


def assemble_kernel(line, cov_ref, hi_ref, mid_ref, low_ref):
    tm = lax.axis_index("tm")
    panel = lax.axis_index("panel")
    low_z = tm // PLANE
    plane = tm % PLANE
    h = pl.program_id(0)
    own_lag = 3 * (tm * 4 + panel)
    width = COLS // 2

    def fill(at, carry):
        spot = h * 8 + at
        out = pl.ds(pl.multiple_of(at * width, LANES), width)
        for offset in range(3):
            start = L * (M - own_lag - offset) + spot * width
            cov_ref[L * offset : L * offset + L, out] = rolled_window(line, start, width)
        return carry

    lax.fori_loop(0, 8, fill, 0)
    base = L * (373 + (low_z - h) * 192 - 12 * plane + 3 * panel)
    window = rolled_window(line, base, 73 * LANES)
    for offset in range(12):
        pieces = [
            window[:, L * (11 - offset + 12 * at) : L * (11 - offset + 12 * at) + ROWS]
            for at in range(PLANE)
        ]
        hi, mid, low = split3(jnp.concatenate(pieces, axis=1))
        at = slice(L * offset, L * offset + L)
        hi_ref[0, at, :] = hi
        mid_ref[0, at, :] = mid
        low_ref[0, at, :] = low


def assemble(line):
    shape = jax.ShapeDtypeStruct((2, 4 * ROWS, COLS), jnp.bfloat16)
    spec = pl.BlockSpec((1, 4 * ROWS, COLS), lambda h: (h, 0, 0))
    return pl.pallas_call(
        assemble_kernel,
        grid=(2,),
        out_shape=(jax.ShapeDtypeStruct((ROWS, M * L), jnp.float32), shape, shape, shape),
        in_specs=[pl.BlockSpec(memory_space=pltpu.VMEM)],
        out_specs=(pl.BlockSpec((ROWS, M * L // 2), lambda h: (0, h)), spec, spec, spec),
        compiler_params=pltpu.CompilerParams(vmem_limit_bytes=62 * 1024 * 1024),
    )(line)


def exact_dot(left, right, contract):
    return lax.dot_general(
        left,
        right,
        (contract, ((), ())),
        precision=exact_precision,
        preferred_element_type=jnp.float32,
    )


def factor(gram):
    rows = lax.broadcasted_iota(jnp.int32, (B, 2 * B), 0)
    lanes = lax.broadcasted_iota(jnp.int32, (B, 2 * B), 1)
    small_rows = lax.broadcasted_iota(jnp.int32, (B, B), 0)
    small_lanes = lax.broadcasted_iota(jnp.int32, (B, B), 1)
    identity = jnp.where(small_rows == small_lanes, 1.0, 0.0).astype(jnp.float32)
    work = jnp.concatenate([gram, identity], axis=1)
    width = 4
    for first in range(0, B, width):
        columns = [
            jnp.broadcast_to(work[:, first + t : first + t + 1], (B, 2 * B)) for t in range(width)
        ]
        for t in range(width):
            k = first + t
            column = columns[t]
            scale = 1.0 / column[k : k + 1, :]
            weight = jnp.where(rows > k, column * scale, 0.0)
            work = work - weight * work[k : k + 1, :]
            for u in range(t + 1, width):
                columns[u] = columns[u] - weight * column[first + u : first + u + 1, :]
    pivots = jnp.sum(jnp.where(rows == lanes, work, 0.0), axis=1, keepdims=True)
    scaled = work * lax.rsqrt(pivots)
    upper = jnp.where(small_lanes >= small_rows, scaled[:, :B], 0.0)
    inverse = jnp.where(small_lanes <= small_rows, scaled[:, B:], 0.0)
    return upper, inverse


PAIR_FIRST = [(0, y) for y in (2, 1, 3)] + [(1, y) for y in (2, 1, 3, 0)]
PAIR_LAST = [(2, y) for y in (2, 1, 3, 0)] + [(3, y) for y in (2, 1, 3, 0)]
FAR_FIRST = [10, 6, 14, 9, 11, 2, 8, 5, 7, 13, 15, 1, 3, 4, 12]


def pack(block):
    return jnp.concatenate([block[:HALF], block[HALF:]], axis=1)


def unpack(block):
    return jnp.concatenate([block[:, :B], block[:, B:]], axis=0)


def lanczos_kernel(
    start_ref,
    hi_ref,
    mid_ref,
    low_ref,
    basis_ref,
    diag_ref,
    off_ref,
    tile_hi,
    tile_mid,
    tile_low,
    work,
    current,
    applied,
    packed,
    gathered,
    stacked,
    accumulated,
    partial,
    landed,
    gram,
    stage1,
    slab,
    stage2,
    total,
    full,
    tile_sem,
    send_q,
    recv_q,
    send_p,
    recv_p,
    send_1,
    recv_1,
    send_2,
    recv_2,
    send_3,
    recv_3,
):
    tm = lax.axis_index("tm")
    panel = lax.axis_index("panel")
    low_z = tm // PLANE
    plane = tm % PLANE
    line = low_z * 4 + panel
    tiles = [
        pltpu.make_async_copy(source, target, tile_sem.at[at])
        for at, (source, target) in enumerate(
            ((hi_ref, tile_hi), (mid_ref, tile_mid), (low_ref, tile_low))
        )
    ]
    for copy in tiles:
        copy.start()

    plane_peer = peers(plane, low_z, panel)

    def line_peer(step):
        spot_z = (low_z + step // 4) % 2
        spot_p = (panel + step % 4) % 4
        return spot_z * 4 + spot_p, (spot_z * PLANE + plane, spot_p)

    pair_at = plane // 8
    odd_x = (plane // 4) % 2

    def x_at(turn):
        side = (pair_at + turn // 2) % 2
        return side * 2 + (odd_x + turn) % 2

    barrier = pltpu.get_barrier_semaphore()
    for step in range(1, PLANE):
        pl.semaphore_signal(barrier, inc=1, device_id=plane_peer(step)[1], device_id_type=MESH)
    for step in range(1, LINE):
        pl.semaphore_signal(barrier, inc=1, device_id=line_peer(step)[1], device_id_type=MESH)
    pl.semaphore_wait(barrier, PLANE + LINE - 2)

    def remote(source, target, send, receive, device):
        return pltpu.make_async_remote_copy(
            src_ref=source,
            dst_ref=target,
            send_sem=send,
            recv_sem=receive,
            device_id=device,
            device_id_type=MESH,
        )

    work[...] = start_ref[...]
    current[...] = jnp.zeros_like(current)
    applied[...] = jnp.zeros_like(applied)

    def one_step(step_at, last):
        slot = step_at % 2
        before = current[...]
        rows_block = work[...]

        def block_copies(places, first):
            found = []
            for at, (turn, y) in enumerate(places):
                to_x = x_at(turn)
                to_y = (plane % 4 + y) % 4
                from_y = (plane % 4 + 4 - y) % 4
                to_spot = to_x * 4 + to_y
                copy = remote(
                    packed,
                    gathered.at[slot, plane],
                    send_q.at[first + at],
                    recv_q.at[slot, first + at],
                    (low_z * PLANE + to_spot, panel),
                )
                found.append((copy, x_at(turn) * 4 + from_y))
            return found

        near = [] if last else block_copies(PAIR_FIRST, 0)
        far = [] if last else block_copies(PAIR_LAST, len(PAIR_FIRST))
        if not last:
            packed[...] = pack(rows_block)
            for copy, _ in near + far:
                copy.start()

        both = jnp.concatenate([before, rows_block], axis=1)
        gram[...] = exact_dot(both, both, ((0,), (0,))).reshape(LINE, 16, 2 * B)
        firsts = [
            remote(
                gram.at[line_peer(step)[0]],
                stage1.at[line],
                send_1.at[step],
                recv_1.at[step],
                line_peer(step)[1],
            )
            for step in range(1, LINE)
        ]
        for copy in firsts:
            copy.start()
        stage1[line] = gram[line]

        def lay(spot, block):
            hi, mid, low = split3(unpack(block))
            at = pl.ds(pl.multiple_of(spot * ROWS, ROWS), ROWS)
            stacked[at, :] = jnp.concatenate([hi, mid, low], axis=1)

        if not last:
            lay(plane, packed[...])
        for copy in firsts:
            copy.wait()
        reduced = stage1[0]
        for spot in range(1, LINE):
            reduced = reduced + stage1[spot]
        slab[...] = reduced
        stage2[slot, plane] = reduced
        seconds = [
            remote(
                slab,
                stage2.at[slot, plane],
                send_2.at[step],
                recv_2.at[slot, step],
                plane_peer(step)[1],
            )
            for step in FAR_FIRST
        ]
        for copy in seconds:
            copy.start()

        sums = [
            remote(
                partial.at[line_peer(step)[0]],
                landed.at[slot, line],
                send_p.at[step],
                recv_p.at[slot, step],
                line_peer(step)[1],
            )
            for step in range(1, LINE)
            if not last
        ]

        def multiply(h, half):
            lanes = pl.ds(pl.multiple_of(half * HALF_COLS, HALF_COLS), HALF_COLS)
            first = jnp.dot(tile_hi[h, :, lanes], stacked[lanes, :], preferred_element_type=jnp.float32)
            second = jnp.dot(
                tile_mid[h, :, lanes], stacked[lanes, : 2 * B], preferred_element_type=jnp.float32
            )
            third = jnp.dot(
                tile_low[h, :, lanes], stacked[lanes, :B], preferred_element_type=jnp.float32
            )
            low_part = third + second[:, B:] + first[:, 2 * B :]
            return first[:, :B] + (first[:, B : 2 * B] + second[:, :B] + low_part)

        def send_sums(h):
            for at, copy in enumerate(sums):
                @pl.when((low_z + (at + 1) // 4) % 2 == h)
                def _():
                    copy.start()

            @pl.when(low_z == h)
            def _():
                landed[slot, line] = partial[line]

        def finish(h):
            product = accumulated[h] + multiply(h, other)
            for spot in range(4):
                rows = product[spot * ROWS : (spot + 1) * ROWS]
                partial[h * 4 + spot] = pack(rows)
            send_sums(h)

        other = 1 - pair_at
        if not last:
            for copy, spot in near:
                copy.wait()
                lay(spot, gathered[slot, spot])

            @pl.when(step_at == 0)
            def _():
                for copy in tiles:
                    copy.wait()

            def begin(h, carry):
                accumulated[h] = multiply(h, pair_at)
                return carry

            lax.fori_loop(0, 2, begin, 0)
            for copy, spot in far:
                copy.wait()
                lay(spot, gathered[slot, spot])
            finish(0)

        for copy in seconds:
            copy.wait()
        reduced = stage2[slot, 0]
        for spot in range(1, PLANE):
            reduced = reduced + stage2[slot, spot]
        total[...] = reduced
        full[line] = reduced
        thirds = [
            remote(total, full.at[line], send_3.at[step], recv_3.at[step], line_peer(step)[1])
            for step in range(1, LINE)
        ]
        for copy in thirds:
            copy.start()
        if not last:
            finish(1)
        for copy in thirds:
            copy.wait()
        summed = full[...].reshape(2 * B, 2 * B)
        basis_gram = summed[:B, :B]
        diagonal = summed[:B, B:]
        work_gram = summed[B:, B:]
        weighted = exact_dot(basis_gram, diagonal, ((1,), (0,)))
        left = exact_dot(diagonal, 2.0 * diagonal - weighted, ((0,), (0,)))
        upper, inverse = factor(work_gram - left)
        diag_ref[jnp.maximum(step_at - 1, 0)] = diagonal
        off_ref[step_at] = upper
        if last:
            reduced = rows_block - exact_dot(before, diagonal, ((1,), (0,)))
            basis_ref[step_at] = exact_dot(reduced, inverse, ((1,), (1,)))
            return
        for copy in sums:
            copy.wait()
        value = landed[slot, 0]
        for spot in range(1, LINE):
            value = value + landed[slot, spot]
        old = jnp.concatenate([before, applied[...]], axis=0)
        new = jnp.concatenate([rows_block, unpack(value)], axis=0)
        reduced = new - exact_dot(old, diagonal, ((1,), (0,)))
        fresh = exact_dot(reduced, inverse, ((1,), (1,)))
        basis_ref[step_at] = fresh[:ROWS]
        current[...] = fresh[:ROWS]
        applied[...] = fresh[ROWS:]
        work[...] = fresh[ROWS:] - exact_dot(before, upper, ((1,), (1,)))

    def body(step_at, carry):
        one_step(step_at, False)
        return carry

    lax.fori_loop(0, ITERS, body, 0)
    one_step(ITERS, True)


def lanczos(start, hi, mid, low):
    vmem = pl.BlockSpec(memory_space=pltpu.VMEM)
    away = pl.BlockSpec(memory_space=pl.ANY)
    dma = pltpu.SemaphoreType.DMA
    tile = pltpu.VMEM((2, 4 * ROWS, COLS), jnp.bfloat16)
    return pl.pallas_call(
        lanczos_kernel,
        out_shape=(
            jax.ShapeDtypeStruct((ITERS + 1, ROWS, B), jnp.float32),
            jax.ShapeDtypeStruct((ITERS, B, B), jnp.float32),
            jax.ShapeDtypeStruct((ITERS + 1, B, B), jnp.float32),
        ),
        in_specs=[vmem, away, away, away],
        out_specs=(vmem, vmem, vmem),
        scratch_shapes=[
            tile,
            tile,
            tile,
            pltpu.VMEM((ROWS, B), jnp.float32),
            pltpu.VMEM((ROWS, B), jnp.float32),
            pltpu.VMEM((ROWS, B), jnp.float32),
            pltpu.VMEM((HALF, 2 * B), jnp.float32),
            pltpu.VMEM((2, PLANE, HALF, 2 * B), jnp.float32),
            pltpu.VMEM((COLS, 3 * B), jnp.bfloat16),
            pltpu.VMEM((2, 4 * ROWS, B), jnp.float32),
            pltpu.VMEM((LINE, HALF, 2 * B), jnp.float32),
            pltpu.VMEM((2, LINE, HALF, 2 * B), jnp.float32),
            pltpu.VMEM((LINE, 16, 2 * B), jnp.float32),
            pltpu.VMEM((LINE, 16, 2 * B), jnp.float32),
            pltpu.VMEM((16, 2 * B), jnp.float32),
            pltpu.VMEM((2, PLANE, 16, 2 * B), jnp.float32),
            pltpu.VMEM((16, 2 * B), jnp.float32),
            pltpu.VMEM((LINE, 16, 2 * B), jnp.float32),
            dma((3,)),
            dma((PLANE,)),
            dma((2, PLANE)),
            dma((LINE,)),
            dma((2, LINE)),
            dma((LINE,)),
            dma((LINE,)),
            dma((PLANE,)),
            dma((2, PLANE)),
            dma((LINE,)),
            dma((LINE,)),
        ],
        compiler_params=pltpu.CompilerParams(
            collective_id=0, has_side_effects=True, vmem_limit_bytes=60 * 1024 * 1024
        ),
    )(start, hi, mid, low)


def local(series, start_block):
    covariance, hi, mid, low = assemble(lag_blocks(series))
    basis, diag, off = lanczos(start_block, hi, mid, low)
    return covariance, basis, diag, off


def solution(mesh):
    placed = (P(None, "tm"), P(("tm", "panel"), None))
    return jax.shard_map(
        local,
        mesh=mesh,
        in_specs=placed,
        out_specs=(P(("tm", "panel"), None), P(None, ("tm", "panel"), None), P(), P()),
        check_vma=False,
    )
```

```python
import functools

import jax
import jax.numpy as jnp
from jax import lax
from jax.experimental import pallas as pl
from jax.experimental.pallas import tpu as pltpu
from jax.sharding import PartitionSpec as P

L = 48
M = 384
B = 64
ITERS = 6
ROWS = 144
HALF = ROWS // 2
PLANE = 16
LINE = 8
COLS = PLANE * ROWS
LANES = 128
DAYS = 256
SPAN = PLANE * DAYS
LAGS = 12

exact_precision = lax.Precision.HIGHEST
MESH = pl.DeviceIdType.MESH


def split3(x):
    hi = x.astype(jnp.bfloat16)
    rest = x - hi.astype(jnp.float32)
    mid = rest.astype(jnp.bfloat16)
    low = (rest - mid.astype(jnp.float32)).astype(jnp.bfloat16)
    return hi, mid, low


def peers(plane, low_z, panel):
    def plane_peer(step):
        spot_x = (plane // 4 + step // 4) % 4
        spot_y = (plane % 4 + step % 4) % 4
        spot = spot_x * 4 + spot_y
        return spot, (low_z * PLANE + spot, panel)

    return plane_peer


def rolled_window(ref, start, width):
    first = start // LANES
    rest = start % LANES
    lanes = lax.broadcasted_iota(jnp.int32, (L, LANES), 1)
    pieces = [
        pltpu.roll(
            ref[:, pl.ds(pl.multiple_of((first + at) * LANES, LANES), LANES)],
            (LANES - rest) % LANES,
            1,
        )
        for at in range(width // LANES + 1)
    ]
    kept = lanes < LANES - rest
    joined = [jnp.where(kept, pieces[at], pieces[at + 1]) for at in range(width // LANES)]
    return jnp.concatenate(joined, axis=1)


def lag_kernel(
    series_ref,
    line,
    blocks,
    flat,
    shifted,
    own,
    win_hi,
    win_mid,
    win_low,
    mine,
    theirs,
    send_s,
    recv_s,
    send_d,
    recv_d,
    send_c,
    recv_c,
    send_f,
    recv_f,
    send_h,
    recv_h,
):
    tm = lax.axis_index("tm")
    panel = lax.axis_index("panel")
    low_z = tm // PLANE
    plane = tm % PLANE
    core = panel % 2
    group = plane * 2 + core
    plane_peer = peers(plane, low_z, panel)
    across = ((1 - low_z) * PLANE + plane, panel)
    beside = (tm, panel + 1 - 2 * core)

    barrier = pltpu.get_barrier_semaphore()
    for step in range(1, PLANE):
        pl.semaphore_signal(barrier, inc=1, device_id=plane_peer(step)[1], device_id_type=MESH)
    pl.semaphore_signal(barrier, inc=1, device_id=across, device_id_type=MESH)
    pl.semaphore_signal(barrier, inc=1, device_id=beside, device_id_type=MESH)
    pl.semaphore_wait(barrier, PLANE + 1)

    def remote(source, target, send, receive, device):
        return pltpu.make_async_remote_copy(
            src_ref=source,
            dst_ref=target,
            send_sem=send,
            recv_sem=receive,
            device_id=device,
            device_id_type=MESH,
        )

    x = plane // 4
    y = plane % 4
    share = L // 2

    def spot_at(turn_x, turn_y):
        return ((x + turn_x) % 4) * 4 + (y + turn_y) % 4

    def chip_at(spot):
        return (low_z * PLANE + spot, panel)

    turns = [(p, q) for p in (2, 1, 3, 0) for q in (2, 1, 3, 0) if p or q]
    rows = pl.ds(pl.multiple_of(core * share, share), share)

    def place(spot):
        return pl.ds(pl.multiple_of(spot * DAYS, DAYS), DAYS)

    flat[:, place(plane)] = series_ref[...]
    days = [
        remote(
            series_ref.at[rows],
            flat.at[rows, place(plane)],
            send_s.at[at],
            recv_s.at[at],
            chip_at(spot_at(*turn)),
        )
        for at, turn in enumerate(turns)
    ]
    for copy in days:
        copy.start()
    shared = []
    for at, turn in enumerate(turns):
        days[at].wait_recv()
        held = flat.at[rows, place(spot_at(-turn[0] + 4, -turn[1] + 4))]
        copy = remote(held, held, send_d.at[at], recv_d.at[at], beside)
        copy.start()
        shared.append(copy)
    for copy in days:
        copy.wait_send()
    for copy in shared:
        copy.wait()
    halo = remote(
        flat.at[:, : 2 * DAYS], flat.at[:, SPAN : SPAN + 2 * DAYS], send_h.at[0], recv_h.at[0], across
    )
    halo.start()
    hi, mid, low = split3(flat[:, :SPAN])
    own[:L] = hi
    own[L : 2 * L] = mid
    own[2 * L :] = low
    halo.wait()
    beyond = flat[:, SPAN : SPAN + 2 * DAYS]
    flat[:, SPAN : SPAN + 2 * DAYS] = jnp.where(low_z == 1, jnp.zeros_like(beyond), beyond)
    shifted[...] = rolled_window(flat, group * LAGS, SPAN + LANES)
    for lag in range(LAGS):
        hi, mid, low = split3(shifted[:, lag : lag + SPAN])
        at = slice(L * lag, L * lag + L)
        win_hi[at, :] = hi
        win_mid[at, :] = mid
        win_low[at, :] = low

    def product(left, right):
        return lax.dot_general(
            left, right, (((1,), (1,)), ((), ())), preferred_element_type=jnp.float32
        )

    first = product(win_hi[...], own[...])
    second = product(win_mid[...], own[: 2 * L])
    third = product(win_low[...], own[:L])
    low_part = first[:, 2 * L :] + second[:, L:] + third
    sums = first[:, :L] + (first[:, L : 2 * L] + second[:, :L] + low_part)
    mine[...] = jnp.transpose(sums)
    half = remote(mine, theirs, send_h.at[1], recv_h.at[1], across)
    half.start()
    lanes = lax.broadcasted_iota(jnp.int32, (L, LAGS * L), 1)
    lag_at = jnp.zeros_like(lanes)
    for lag in range(1, LAGS):
        lag_at = lag_at + jnp.where(lanes >= lag * L, 1, 0)
    counts = (2 * SPAN - (group * LAGS + lag_at)).astype(jnp.float32)
    half.wait()
    blocks[group] = (mine[...] + theirs[...]) / counts

    def held(spot, color):
        return blocks.at[spot * 2 + core, pl.ds(color * share, share)]

    started = []

    def forward(origin_x, origin_y, color, along, to_turn):
        to_x, to_y = (to_turn, 0) if along == 0 else (0, to_turn)
        source = held(spot_at(4 - origin_x, 4 - origin_y), color)
        key = (origin_x + to_x) % 4 * 4 + (origin_y + to_y) % 4
        copy = remote(
            source,
            source,
            send_c.at[color, key],
            recv_c.at[color, key],
            chip_at(spot_at(to_x, to_y)),
        )
        copy.start()
        started.append(copy)

    def landed(origin_x, origin_y, color):
        key = origin_x * 4 + origin_y
        part = held(spot_at(4 - origin_x, 4 - origin_y), color)
        remote(part, part, send_c.at[color, key], recv_c.at[color, key], chip_at(plane)).wait_recv()
        give(origin_x, origin_y, color)

    def give(origin_x, origin_y, color):
        key = origin_x * 4 + origin_y
        part = held(spot_at(4 - origin_x, 4 - origin_y), color)
        copy = remote(part, part, send_f.at[color, key], recv_f.at[color, key], beside)
        copy.start()
        passed[color, key] = copy

    passed = {}
    for turn in (2, 1, 3):
        forward(0, 0, 0, 0, turn)
        forward(0, 0, 1, 1, turn)
    for turn in (2, 1, 3):
        forward(0, 0, 0, 1, turn)
        forward(0, 0, 1, 0, turn)
    for color in range(2):
        give(0, 0, color)

    lanes = lax.broadcasted_iota(jnp.int32, (L, LANES), 1)
    pair = 2 * LAGS * L

    def lay(at):
        both = jnp.concatenate([blocks[2 * at], blocks[2 * at + 1]], axis=1)
        line[:, pl.ds(pl.multiple_of(M * L + at * pair, LANES), pair)] = both
        turned = jnp.transpose(both)
        parts = [turned[L * lag : L * lag + L, :] for lag in range(2 * LAGS - 1, -1, -1)]
        filler = jnp.zeros((L, L), jnp.float32)
        tail = jnp.zeros((L, LANES - L), jnp.float32)
        wide = jnp.concatenate([filler] + parts + [tail], axis=1)
        start = (PLANE - 1 - at) * pair
        front = pl.ds(pl.multiple_of(start, LANES), LANES)
        inner = pl.ds(pl.multiple_of(start + LANES, LANES), pair - LANES)
        back = pl.ds(pl.multiple_of(start + pair, LANES), LANES)
        line[:, front] = jnp.where(lanes < L, line[:, front], wide[:, :LANES])
        line[:, inner] = wide[:, LANES:pair]

        @pl.when(at > 0)
        def _():
            line[:, back] = jnp.where(lanes < L, wide[:, pair:], line[:, back])

    def settle(origin_x, origin_y):
        key = origin_x * 4 + origin_y
        for color in range(2):
            passed[color, key].wait()
        lay(spot_at(4 - origin_x, 4 - origin_y))

    first_wave = (1, 3, 2)
    for turn in first_wave:
        landed(turn, 0, 0)
        for to_turn in (2, 1, 3):
            forward(turn, 0, 0, 1, to_turn)
        landed(0, turn, 1)
        for to_turn in (2, 1, 3):
            forward(0, turn, 1, 0, to_turn)
    settle(0, 0)
    for turn in first_wave:
        landed(0, turn, 0)
        landed(turn, 0, 1)
        settle(0, turn)
        settle(turn, 0)
    for turn_x in first_wave:
        for turn_y in first_wave:
            landed(turn_x, turn_y, 0)
            landed(turn_x, turn_y, 1)
            settle(turn_x, turn_y)
    for copy in started:
        copy.wait_send()


def lag_blocks(series):
    vmem = pl.BlockSpec(memory_space=pltpu.VMEM)
    dma = pltpu.SemaphoreType.DMA
    return pl.pallas_call(
        lag_kernel,
        out_shape=jax.ShapeDtypeStruct((L, 2 * M * L + 2 * LANES), jnp.float32),
        in_specs=[vmem],
        out_specs=vmem,
        scratch_shapes=[
            pltpu.VMEM((2 * PLANE, L, LAGS * L), jnp.float32),
            pltpu.VMEM((L, SPAN + 2 * DAYS), jnp.float32),
            pltpu.VMEM((L, SPAN + LANES), jnp.float32),
            pltpu.VMEM((3 * L, SPAN), jnp.bfloat16),
            pltpu.VMEM((LAGS * L, SPAN), jnp.bfloat16),
            pltpu.VMEM((LAGS * L, SPAN), jnp.bfloat16),
            pltpu.VMEM((LAGS * L, SPAN), jnp.bfloat16),
            pltpu.VMEM((L, LAGS * L), jnp.float32),
            pltpu.VMEM((L, LAGS * L), jnp.float32),
            dma((PLANE,)),
            dma((PLANE,)),
            dma((PLANE,)),
            dma((PLANE,)),
            dma((2, PLANE)),
            dma((2, PLANE)),
            dma((2, PLANE)),
            dma((2, PLANE)),
            dma((2,)),
            dma((2,)),
        ],
        compiler_params=pltpu.CompilerParams(
            collective_id=1, has_side_effects=True, vmem_limit_bytes=60 * 1024 * 1024
        ),
    )(series)


def assemble_kernel(line, cov_ref, hi_ref, mid_ref, low_ref):
    tm = lax.axis_index("tm")
    panel = lax.axis_index("panel")
    low_z = tm // PLANE
    plane = tm % PLANE
    h = pl.program_id(0)
    own_lag = 3 * (tm * 4 + panel)
    width = COLS // 2

    def fill(at, carry):
        spot = h * 8 + at
        out = pl.ds(pl.multiple_of(at * width, LANES), width)
        for offset in range(3):
            start = L * (M - own_lag - offset) + spot * width
            cov_ref[L * offset : L * offset + L, out] = rolled_window(line, start, width)
        return carry

    lax.fori_loop(0, 8, fill, 0)
    base = L * (373 + (low_z - h) * 192 - 12 * plane + 3 * panel)
    window = rolled_window(line, base, 73 * LANES)
    for offset in range(12):
        pieces = [
            window[:, L * (11 - offset + 12 * at) : L * (11 - offset + 12 * at) + ROWS]
            for at in range(PLANE)
        ]
        hi, mid, low = split3(jnp.concatenate(pieces, axis=1))
        at = slice(L * offset, L * offset + L)
        hi_ref[0, at, :] = hi
        mid_ref[0, at, :] = mid
        low_ref[0, at, :] = low


def assemble(line):
    shape = jax.ShapeDtypeStruct((2, 4 * ROWS, COLS), jnp.bfloat16)
    spec = pl.BlockSpec((1, 4 * ROWS, COLS), lambda h: (h, 0, 0))
    return pl.pallas_call(
        assemble_kernel,
        grid=(2,),
        out_shape=(jax.ShapeDtypeStruct((ROWS, M * L), jnp.float32), shape, shape, shape),
        in_specs=[pl.BlockSpec(memory_space=pltpu.VMEM)],
        out_specs=(pl.BlockSpec((ROWS, M * L // 2), lambda h: (0, h)), spec, spec, spec),
        compiler_params=pltpu.CompilerParams(vmem_limit_bytes=62 * 1024 * 1024),
    )(line)


def exact_dot(left, right, contract):
    return lax.dot_general(
        left,
        right,
        (contract, ((), ())),
        precision=exact_precision,
        preferred_element_type=jnp.float32,
    )


def factor(gram):
    rows = lax.broadcasted_iota(jnp.int32, (B, 2 * B), 0)
    lanes = lax.broadcasted_iota(jnp.int32, (B, 2 * B), 1)
    small_rows = lax.broadcasted_iota(jnp.int32, (B, B), 0)
    small_lanes = lax.broadcasted_iota(jnp.int32, (B, B), 1)
    identity = jnp.where(small_rows == small_lanes, 1.0, 0.0).astype(jnp.float32)
    work = jnp.concatenate([gram, identity], axis=1)
    width = 8
    for first in range(0, B, width):
        columns = [
            jnp.broadcast_to(work[:, first + t : first + t + 1], (B, 2 * B)) for t in range(width)
        ]
        for t in range(width):
            k = first + t
            column = columns[t]
            scale = 1.0 / column[k : k + 1, :]
            weight = jnp.where(rows > k, column * scale, 0.0)
            work = work - weight * work[k : k + 1, :]
            for u in range(t + 1, width):
                columns[u] = columns[u] - weight * column[first + u : first + u + 1, :]
    pivots = jnp.sum(jnp.where(rows == lanes, work, 0.0), axis=1, keepdims=True)
    scaled = work * lax.rsqrt(pivots)
    upper = jnp.where(small_lanes >= small_rows, scaled[:, :B], 0.0)
    inverse = jnp.where(small_lanes <= small_rows, scaled[:, B:], 0.0)
    return upper, inverse


FAR_FIRST = [10, 6, 14, 9, 11, 2, 8, 5, 7, 13, 15, 1, 3, 4, 12]


def pack(block):
    return jnp.concatenate([block[:HALF], block[HALF:]], axis=1)


def unpack(block):
    return jnp.concatenate([block[:, :B], block[:, B:]], axis=0)


def lanczos_kernel(
    start_ref,
    hi_ref,
    mid_ref,
    low_ref,
    basis_ref,
    diag_ref,
    off_ref,
    tile_hi,
    tile_mid,
    tile_low,
    work,
    current,
    applied,
    gathered,
    stacked,
    partial,
    landed,
    gram,
    stage1,
    slab,
    stage2,
    total,
    full,
    tile_sem,
    send_q,
    recv_q,
    send_p,
    recv_p,
    send_1,
    recv_1,
    send_2,
    recv_2,
    send_3,
    recv_3,
):
    tm = lax.axis_index("tm")
    panel = lax.axis_index("panel")
    low_z = tm // PLANE
    plane = tm % PLANE
    line = low_z * 4 + panel
    tiles = [
        pltpu.make_async_copy(source, target, tile_sem.at[at])
        for at, (source, target) in enumerate(
            ((hi_ref, tile_hi), (mid_ref, tile_mid), (low_ref, tile_low))
        )
    ]
    for copy in tiles:
        copy.start()

    plane_peer = peers(plane, low_z, panel)

    def line_peer(step):
        spot_z = (low_z + step // 4) % 2
        spot_p = (panel + step % 4) % 4
        return spot_z * 4 + spot_p, (spot_z * PLANE + plane, spot_p)

    barrier = pltpu.get_barrier_semaphore()
    for step in range(1, PLANE):
        pl.semaphore_signal(barrier, inc=1, device_id=plane_peer(step)[1], device_id_type=MESH)
    for step in range(1, LINE):
        pl.semaphore_signal(barrier, inc=1, device_id=line_peer(step)[1], device_id_type=MESH)
    pl.semaphore_wait(barrier, PLANE + LINE - 2)

    def remote(source, target, send, receive, device):
        return pltpu.make_async_remote_copy(
            src_ref=source,
            dst_ref=target,
            send_sem=send,
            recv_sem=receive,
            device_id=device,
            device_id_type=MESH,
        )

    work[...] = start_ref[...]
    current[...] = jnp.zeros_like(current)
    applied[...] = jnp.zeros_like(applied)

    def one_step(step_at, last):
        slot = step_at % 2
        before = current[...]
        rows_block = work[...]

        moved = []

        def part_at(spot, color):
            return gathered.at[slot, spot, pl.ds(40 * color, 40 - 8 * color)]

        def spot_at(turn_x, turn_y):
            return ((plane // 4 + turn_x) % 4) * 4 + (plane % 4 + turn_y) % 4

        def forward(origin_x, origin_y, color, along, to_turn):
            to_x, to_y = (to_turn, 0) if along == 0 else (0, to_turn)
            part = part_at(spot_at(4 - origin_x, 4 - origin_y), color)
            key = (origin_x + to_x) % 4 * 4 + (origin_y + to_y) % 4
            copy = remote(
                part,
                part,
                send_q.at[color, key],
                recv_q.at[slot, color, key],
                (low_z * PLANE + spot_at(to_x, to_y), panel),
            )
            copy.start()
            moved.append(copy)

        def await_part(origin_x, origin_y, color):
            key = origin_x * 4 + origin_y
            part = part_at(spot_at(4 - origin_x, 4 - origin_y), color)
            remote(
                part, part, send_q.at[color, key], recv_q.at[slot, color, key], (tm, panel)
            ).wait_recv()

        if not last:
            gathered[slot, plane] = pack(rows_block)
            for turn in (2, 1, 3):
                forward(0, 0, 0, 0, turn)
                forward(0, 0, 1, 1, turn)
            for turn in (2, 1, 3):
                forward(0, 0, 0, 1, turn)
                forward(0, 0, 1, 0, turn)

        both = jnp.concatenate([before, rows_block], axis=1)
        gram[...] = exact_dot(both, both, ((0,), (0,))).reshape(LINE, 16, 2 * B)
        firsts = [
            remote(
                gram.at[line_peer(step)[0]],
                stage1.at[line],
                send_1.at[step],
                recv_1.at[step],
                line_peer(step)[1],
            )
            for step in range(1, LINE)
        ]
        for copy in firsts:
            copy.start()
        stage1[line] = gram[line]

        def lay(spot, block):
            hi, mid, low = split3(unpack(block))
            at = pl.ds(pl.multiple_of(spot * ROWS, ROWS), ROWS)
            stacked[at, :] = jnp.concatenate([hi, mid, low], axis=1)

        wave = (1, 3, 2)
        if not last:
            lay(plane, gathered[slot, plane])
            for turn in wave:
                await_part(turn, 0, 0)
                for to_turn in (2, 1, 3):
                    forward(turn, 0, 0, 1, to_turn)
                await_part(0, turn, 1)
                for to_turn in (2, 1, 3):
                    forward(0, turn, 1, 0, to_turn)
        for copy in firsts:
            copy.wait()
        reduced = stage1[0]
        for spot in range(1, LINE):
            reduced = reduced + stage1[spot]
        slab[...] = reduced
        stage2[slot, plane] = reduced
        seconds = [
            remote(
                slab,
                stage2.at[slot, plane],
                send_2.at[step],
                recv_2.at[slot, step],
                plane_peer(step)[1],
            )
            for step in FAR_FIRST
        ]
        for copy in seconds:
            copy.start()

        sums = [
            remote(
                partial.at[line_peer(step)[0]],
                landed.at[slot, line],
                send_p.at[step],
                recv_p.at[slot, step],
                line_peer(step)[1],
            )
            for step in range(1, LINE)
            if not last
        ]

        def multiply(h):
            first = jnp.dot(tile_hi[h], stacked[...], preferred_element_type=jnp.float32)
            second = jnp.dot(
                tile_mid[h], stacked[:, : 2 * B], preferred_element_type=jnp.float32
            )
            third = jnp.dot(tile_low[h], stacked[:, :B], preferred_element_type=jnp.float32)
            low_part = third + second[:, B:] + first[:, 2 * B :]
            return first[:, :B] + (first[:, B : 2 * B] + second[:, :B] + low_part)

        def send_sums(h):
            for at, copy in enumerate(sums):
                @pl.when((low_z + (at + 1) // 4) % 2 == h)
                def _():
                    copy.start()

            @pl.when(low_z == h)
            def _():
                landed[slot, line] = partial[line]

        def finish(h):
            product = multiply(h)
            for spot in range(4):
                rows = product[spot * ROWS : (spot + 1) * ROWS]
                partial[h * 4 + spot] = pack(rows)
            send_sums(h)

        def place(origin_x, origin_y):
            spot = spot_at(4 - origin_x, 4 - origin_y)
            lay(spot, gathered[slot, spot])

        if not last:
            for turn in wave:
                await_part(0, turn, 0)
                await_part(turn, 0, 1)
                place(0, turn)
                place(turn, 0)
            for turn_x in wave:
                for turn_y in wave:
                    await_part(turn_x, turn_y, 0)
                    await_part(turn_x, turn_y, 1)
                    place(turn_x, turn_y)

            @pl.when(step_at == 0)
            def _():
                for copy in tiles:
                    copy.wait()

            finish(0)

        for copy in seconds:
            copy.wait()
        reduced = stage2[slot, 0]
        for spot in range(1, PLANE):
            reduced = reduced + stage2[slot, spot]
        total[...] = reduced
        full[line] = reduced
        thirds = [
            remote(total, full.at[line], send_3.at[step], recv_3.at[step], line_peer(step)[1])
            for step in range(1, LINE)
        ]
        for copy in thirds:
            copy.start()
        if not last:
            finish(1)
        for copy in thirds:
            copy.wait()
        summed = full[...].reshape(2 * B, 2 * B)
        basis_gram = summed[:B, :B]
        diagonal = summed[:B, B:]
        work_gram = summed[B:, B:]
        weighted = exact_dot(basis_gram, diagonal, ((1,), (0,)))
        left = exact_dot(diagonal, 2.0 * diagonal - weighted, ((0,), (0,)))
        upper, inverse = factor(work_gram - left)
        diag_ref[jnp.maximum(step_at - 1, 0)] = diagonal
        off_ref[step_at] = upper
        if last:
            reduced = rows_block - exact_dot(before, diagonal, ((1,), (0,)))
            basis_ref[step_at] = exact_dot(reduced, inverse, ((1,), (1,)))
            return
        for copy in sums:
            copy.wait()
        for copy in moved:
            copy.wait_send()
        value = landed[slot, 0]
        for spot in range(1, LINE):
            value = value + landed[slot, spot]
        old = jnp.concatenate([before, applied[...]], axis=0)
        new = jnp.concatenate([rows_block, unpack(value)], axis=0)
        reduced = new - exact_dot(old, diagonal, ((1,), (0,)))
        fresh = exact_dot(reduced, inverse, ((1,), (1,)))
        basis_ref[step_at] = fresh[:ROWS]
        current[...] = fresh[:ROWS]
        applied[...] = fresh[ROWS:]
        work[...] = fresh[ROWS:] - exact_dot(before, upper, ((1,), (1,)))

    def body(step_at, carry):
        one_step(step_at, False)
        return carry

    lax.fori_loop(0, ITERS, body, 0)
    one_step(ITERS, True)


def lanczos(start, hi, mid, low):
    vmem = pl.BlockSpec(memory_space=pltpu.VMEM)
    away = pl.BlockSpec(memory_space=pl.ANY)
    dma = pltpu.SemaphoreType.DMA
    tile = pltpu.VMEM((2, 4 * ROWS, COLS), jnp.bfloat16)
    return pl.pallas_call(
        lanczos_kernel,
        out_shape=(
            jax.ShapeDtypeStruct((ITERS + 1, ROWS, B), jnp.float32),
            jax.ShapeDtypeStruct((ITERS, B, B), jnp.float32),
            jax.ShapeDtypeStruct((ITERS + 1, B, B), jnp.float32),
        ),
        in_specs=[vmem, away, away, away],
        out_specs=(vmem, vmem, vmem),
        scratch_shapes=[
            tile,
            tile,
            tile,
            pltpu.VMEM((ROWS, B), jnp.float32),
            pltpu.VMEM((ROWS, B), jnp.float32),
            pltpu.VMEM((ROWS, B), jnp.float32),
            pltpu.VMEM((2, PLANE, HALF, 2 * B), jnp.float32),
            pltpu.VMEM((COLS, 3 * B), jnp.bfloat16),
            pltpu.VMEM((LINE, HALF, 2 * B), jnp.float32),
            pltpu.VMEM((2, LINE, HALF, 2 * B), jnp.float32),
            pltpu.VMEM((LINE, 16, 2 * B), jnp.float32),
            pltpu.VMEM((LINE, 16, 2 * B), jnp.float32),
            pltpu.VMEM((16, 2 * B), jnp.float32),
            pltpu.VMEM((2, PLANE, 16, 2 * B), jnp.float32),
            pltpu.VMEM((16, 2 * B), jnp.float32),
            pltpu.VMEM((LINE, 16, 2 * B), jnp.float32),
            dma((3,)),
            dma((2, PLANE)),
            dma((2, 2, PLANE)),
            dma((LINE,)),
            dma((2, LINE)),
            dma((LINE,)),
            dma((LINE,)),
            dma((PLANE,)),
            dma((2, PLANE)),
            dma((LINE,)),
            dma((LINE,)),
        ],
        compiler_params=pltpu.CompilerParams(
            collective_id=0, has_side_effects=True, vmem_limit_bytes=60 * 1024 * 1024
        ),
    )(start, hi, mid, low)


def local(series, start_block):
    covariance, hi, mid, low = assemble(lag_blocks(series))
    basis, diag, off = lanczos(start_block, hi, mid, low)
    return covariance, basis, diag, off


def solution(mesh):
    placed = (P(None, "tm"), P(("tm", "panel"), None))
    return jax.shard_map(
        local,
        mesh=mesh,
        in_specs=placed,
        out_specs=(P(("tm", "panel"), None), P(None, ("tm", "panel"), None), P(), P()),
        check_vma=False,
    )
```

```python
import functools

import jax
import jax.numpy as jnp
from jax import lax
from jax.experimental import pallas as pl
from jax.experimental.pallas import tpu as pltpu
from jax.sharding import PartitionSpec as P

L = 48
M = 384
B = 64
ITERS = 6
ROWS = 144
HALF = ROWS // 2
PLANE = 16
LINE = 8
COLS = PLANE * ROWS
LANES = 128
DAYS = 256
SPAN = PLANE * DAYS
LAGS = 12

exact_precision = lax.Precision.HIGHEST
MESH = pl.DeviceIdType.MESH


def split3(x):
    hi = x.astype(jnp.bfloat16)
    rest = x - hi.astype(jnp.float32)
    mid = rest.astype(jnp.bfloat16)
    low = (rest - mid.astype(jnp.float32)).astype(jnp.bfloat16)
    return hi, mid, low


def peers(plane, low_z, panel):
    def plane_peer(step):
        spot_x = (plane // 4 + step // 4) % 4
        spot_y = (plane % 4 + step % 4) % 4
        spot = spot_x * 4 + spot_y
        return spot, (low_z * PLANE + spot, panel)

    return plane_peer


def rolled_window(ref, start, width):
    first = start // LANES
    rest = start % LANES
    lanes = lax.broadcasted_iota(jnp.int32, (L, LANES), 1)
    pieces = [
        pltpu.roll(
            ref[:, pl.ds(pl.multiple_of((first + at) * LANES, LANES), LANES)],
            (LANES - rest) % LANES,
            1,
        )
        for at in range(width // LANES + 1)
    ]
    kept = lanes < LANES - rest
    joined = [jnp.where(kept, pieces[at], pieces[at + 1]) for at in range(width // LANES)]
    return jnp.concatenate(joined, axis=1)


def lag_kernel(
    series_ref,
    line,
    blocks,
    flat,
    shifted,
    own,
    win_hi,
    win_mid,
    win_low,
    mine,
    theirs,
    send_s,
    recv_s,
    send_d,
    recv_d,
    send_c,
    recv_c,
    send_f,
    recv_f,
    send_h,
    recv_h,
):
    tm = lax.axis_index("tm")
    panel = lax.axis_index("panel")
    low_z = tm // PLANE
    plane = tm % PLANE
    core = panel % 2
    group = plane * 2 + core
    plane_peer = peers(plane, low_z, panel)
    across = ((1 - low_z) * PLANE + plane, panel)
    beside = (tm, panel + 1 - 2 * core)

    barrier = pltpu.get_barrier_semaphore()
    for step in range(1, PLANE):
        pl.semaphore_signal(barrier, inc=1, device_id=plane_peer(step)[1], device_id_type=MESH)
    pl.semaphore_signal(barrier, inc=1, device_id=across, device_id_type=MESH)
    pl.semaphore_signal(barrier, inc=1, device_id=beside, device_id_type=MESH)
    pl.semaphore_wait(barrier, PLANE + 1)

    def remote(source, target, send, receive, device):
        return pltpu.make_async_remote_copy(
            src_ref=source,
            dst_ref=target,
            send_sem=send,
            recv_sem=receive,
            device_id=device,
            device_id_type=MESH,
        )

    x = plane // 4
    y = plane % 4
    share = L // 2

    def spot_at(turn_x, turn_y):
        return ((x + turn_x) % 4) * 4 + (y + turn_y) % 4

    def chip_at(spot):
        return (low_z * PLANE + spot, panel)

    turns = [(p, q) for p in (2, 1, 3, 0) for q in (2, 1, 3, 0) if p or q]
    rows = pl.ds(pl.multiple_of(core * share, share), share)

    def place(spot):
        return pl.ds(pl.multiple_of(spot * DAYS, DAYS), DAYS)

    flat[:, place(plane)] = series_ref[...]
    days = [
        remote(
            series_ref.at[rows],
            flat.at[rows, place(plane)],
            send_s.at[at],
            recv_s.at[at],
            chip_at(spot_at(*turn)),
        )
        for at, turn in enumerate(turns)
    ]
    for copy in days:
        copy.start()
    shared = []
    for at, turn in enumerate(turns):
        days[at].wait_recv()
        held = flat.at[rows, place(spot_at(-turn[0] + 4, -turn[1] + 4))]
        copy = remote(held, held, send_d.at[at], recv_d.at[at], beside)
        copy.start()
        shared.append(copy)
    for copy in days:
        copy.wait_send()
    for copy in shared:
        copy.wait()
    halo = remote(
        flat.at[:, : 2 * DAYS], flat.at[:, SPAN : SPAN + 2 * DAYS], send_h.at[0], recv_h.at[0], across
    )
    halo.start()
    hi, mid, low = split3(flat[:, :SPAN])
    own[:L] = hi
    own[L : 2 * L] = mid
    own[2 * L :] = low
    halo.wait()
    beyond = flat[:, SPAN : SPAN + 2 * DAYS]
    flat[:, SPAN : SPAN + 2 * DAYS] = jnp.where(low_z == 1, jnp.zeros_like(beyond), beyond)
    shifted[...] = rolled_window(flat, group * LAGS, SPAN + LANES)
    for lag in range(LAGS):
        hi, mid, low = split3(shifted[:, lag : lag + SPAN])
        at = slice(L * lag, L * lag + L)
        win_hi[at, :] = hi
        win_mid[at, :] = mid
        win_low[at, :] = low

    def product(left, right):
        return lax.dot_general(
            left, right, (((1,), (1,)), ((), ())), preferred_element_type=jnp.float32
        )

    first = product(win_hi[...], own[...])
    second = product(win_mid[...], own[: 2 * L])
    third = product(win_low[...], own[:L])
    low_part = first[:, 2 * L :] + second[:, L:] + third
    sums = first[:, :L] + (first[:, L : 2 * L] + second[:, :L] + low_part)
    mine[...] = jnp.transpose(sums)
    half = remote(mine, theirs, send_h.at[1], recv_h.at[1], across)
    half.start()
    lanes = lax.broadcasted_iota(jnp.int32, (L, LAGS * L), 1)
    lag_at = jnp.zeros_like(lanes)
    for lag in range(1, LAGS):
        lag_at = lag_at + jnp.where(lanes >= lag * L, 1, 0)
    counts = (2 * SPAN - (group * LAGS + lag_at)).astype(jnp.float32)
    half.wait()
    blocks[group] = (mine[...] + theirs[...]) / counts

    def held(spot, color):
        return blocks.at[spot * 2 + core, pl.ds(color * share, share)]

    started = []

    def forward(origin_x, origin_y, color, along, to_turn):
        to_x, to_y = (to_turn, 0) if along == 0 else (0, to_turn)
        source = held(spot_at(4 - origin_x, 4 - origin_y), color)
        key = (origin_x + to_x) % 4 * 4 + (origin_y + to_y) % 4
        copy = remote(
            source,
            source,
            send_c.at[color, key],
            recv_c.at[color, key],
            chip_at(spot_at(to_x, to_y)),
        )
        copy.start()
        started.append(copy)

    def landed(origin_x, origin_y, color):
        key = origin_x * 4 + origin_y
        part = held(spot_at(4 - origin_x, 4 - origin_y), color)
        remote(part, part, send_c.at[color, key], recv_c.at[color, key], chip_at(plane)).wait_recv()
        give(origin_x, origin_y, color)

    def give(origin_x, origin_y, color):
        key = origin_x * 4 + origin_y
        part = held(spot_at(4 - origin_x, 4 - origin_y), color)
        copy = remote(part, part, send_f.at[color, key], recv_f.at[color, key], beside)
        copy.start()
        passed[color, key] = copy

    passed = {}
    for turn in (3, 1):
        forward(0, 0, 0, 0, turn)
        forward(0, 0, 1, 1, turn)
    for turn in (3, 1):
        forward(0, 0, 0, 1, turn)
        forward(0, 0, 1, 0, turn)
    for color in range(2):
        give(0, 0, color)

    lanes = lax.broadcasted_iota(jnp.int32, (L, LANES), 1)
    pair = 2 * LAGS * L

    def lay(at):
        both = jnp.concatenate([blocks[2 * at], blocks[2 * at + 1]], axis=1)
        line[:, pl.ds(pl.multiple_of(M * L + at * pair, LANES), pair)] = both
        turned = jnp.transpose(both)
        parts = [turned[L * lag : L * lag + L, :] for lag in range(2 * LAGS - 1, -1, -1)]
        filler = jnp.zeros((L, L), jnp.float32)
        tail = jnp.zeros((L, LANES - L), jnp.float32)
        wide = jnp.concatenate([filler] + parts + [tail], axis=1)
        start = (PLANE - 1 - at) * pair
        front = pl.ds(pl.multiple_of(start, LANES), LANES)
        inner = pl.ds(pl.multiple_of(start + LANES, LANES), pair - LANES)
        back = pl.ds(pl.multiple_of(start + pair, LANES), LANES)
        line[:, front] = jnp.where(lanes < L, line[:, front], wide[:, :LANES])
        line[:, inner] = wide[:, LANES:pair]

        @pl.when(at > 0)
        def _():
            line[:, back] = jnp.where(lanes < L, wide[:, pair:], line[:, back])

    def settle(origin_x, origin_y):
        key = origin_x * 4 + origin_y
        for color in range(2):
            passed[color, key].wait()
        lay(spot_at(4 - origin_x, 4 - origin_y))

    first_wave = (3, 1, 2)
    for turn in first_wave:
        landed(turn, 0, 0)
        landed(0, turn, 1)
        if turn == 3:
            forward(3, 0, 0, 0, 3)
            forward(0, 3, 1, 1, 3)
        for to_turn in (3, 1):
            forward(turn, 0, 0, 1, to_turn)
            forward(0, turn, 1, 0, to_turn)
        if turn == 3:
            landed(0, 3, 0)
            forward(0, 3, 0, 1, 3)
            landed(3, 0, 1)
            forward(3, 0, 1, 0, 3)
    settle(0, 0)
    for turn in first_wave:
        landed(turn, 3, 0)
        forward(turn, 3, 0, 1, 3)
        landed(3, turn, 1)
        forward(3, turn, 1, 0, 3)
    settle(0, 3)
    settle(3, 0)
    for turn in (1, 2):
        landed(0, turn, 0)
        landed(turn, 0, 1)
        settle(0, turn)
        settle(turn, 0)
    for turn_x in first_wave:
        for turn_y in first_wave:
            if turn_y != 3:
                landed(turn_x, turn_y, 0)
            if turn_x != 3:
                landed(turn_x, turn_y, 1)
            settle(turn_x, turn_y)
    for copy in started:
        copy.wait_send()


def lag_blocks(series):
    vmem = pl.BlockSpec(memory_space=pltpu.VMEM)
    dma = pltpu.SemaphoreType.DMA
    return pl.pallas_call(
        lag_kernel,
        out_shape=jax.ShapeDtypeStruct((L, 2 * M * L + 2 * LANES), jnp.float32),
        in_specs=[vmem],
        out_specs=vmem,
        scratch_shapes=[
            pltpu.VMEM((2 * PLANE, L, LAGS * L), jnp.float32),
            pltpu.VMEM((L, SPAN + 2 * DAYS), jnp.float32),
            pltpu.VMEM((L, SPAN + LANES), jnp.float32),
            pltpu.VMEM((3 * L, SPAN), jnp.bfloat16),
            pltpu.VMEM((LAGS * L, SPAN), jnp.bfloat16),
            pltpu.VMEM((LAGS * L, SPAN), jnp.bfloat16),
            pltpu.VMEM((LAGS * L, SPAN), jnp.bfloat16),
            pltpu.VMEM((L, LAGS * L), jnp.float32),
            pltpu.VMEM((L, LAGS * L), jnp.float32),
            dma((PLANE,)),
            dma((PLANE,)),
            dma((PLANE,)),
            dma((PLANE,)),
            dma((2, PLANE)),
            dma((2, PLANE)),
            dma((2, PLANE)),
            dma((2, PLANE)),
            dma((2,)),
            dma((2,)),
        ],
        compiler_params=pltpu.CompilerParams(
            collective_id=1, has_side_effects=True, vmem_limit_bytes=60 * 1024 * 1024
        ),
    )(series)


def assemble_kernel(line, cov_ref, hi_ref, mid_ref, low_ref):
    tm = lax.axis_index("tm")
    panel = lax.axis_index("panel")
    low_z = tm // PLANE
    plane = tm % PLANE
    h = pl.program_id(0)
    own_lag = 3 * (tm * 4 + panel)
    width = COLS // 2

    def fill(at, carry):
        spot = h * 8 + at
        out = pl.ds(pl.multiple_of(at * width, LANES), width)
        for offset in range(3):
            start = L * (M - own_lag - offset) + spot * width
            cov_ref[L * offset : L * offset + L, out] = rolled_window(line, start, width)
        return carry

    lax.fori_loop(0, 8, fill, 0)
    base = L * (373 + (low_z - h) * 192 - 12 * plane + 3 * panel)
    window = rolled_window(line, base, 73 * LANES)
    for offset in range(12):
        pieces = [
            window[:, L * (11 - offset + 12 * at) : L * (11 - offset + 12 * at) + ROWS]
            for at in range(PLANE)
        ]
        hi, mid, low = split3(jnp.concatenate(pieces, axis=1))
        at = slice(L * offset, L * offset + L)
        hi_ref[0, at, :] = hi
        mid_ref[0, at, :] = mid
        low_ref[0, at, :] = low


def assemble(line):
    shape = jax.ShapeDtypeStruct((2, 4 * ROWS, COLS), jnp.bfloat16)
    spec = pl.BlockSpec((1, 4 * ROWS, COLS), lambda h: (h, 0, 0))
    return pl.pallas_call(
        assemble_kernel,
        grid=(2,),
        out_shape=(jax.ShapeDtypeStruct((ROWS, M * L), jnp.float32), shape, shape, shape),
        in_specs=[pl.BlockSpec(memory_space=pltpu.VMEM)],
        out_specs=(pl.BlockSpec((ROWS, M * L // 2), lambda h: (0, h)), spec, spec, spec),
        compiler_params=pltpu.CompilerParams(vmem_limit_bytes=62 * 1024 * 1024),
    )(line)


def exact_dot(left, right, contract):
    return lax.dot_general(
        left,
        right,
        (contract, ((), ())),
        precision=exact_precision,
        preferred_element_type=jnp.float32,
    )


def factor(gram):
    rows = lax.broadcasted_iota(jnp.int32, (B, 2 * B), 0)
    lanes = lax.broadcasted_iota(jnp.int32, (B, 2 * B), 1)
    small_rows = lax.broadcasted_iota(jnp.int32, (B, B), 0)
    small_lanes = lax.broadcasted_iota(jnp.int32, (B, B), 1)
    identity = jnp.where(small_rows == small_lanes, 1.0, 0.0).astype(jnp.float32)
    work = jnp.concatenate([gram, identity], axis=1)
    width = 8
    for first in range(0, B, width):
        columns = [
            jnp.broadcast_to(work[:, first + t : first + t + 1], (B, 2 * B)) for t in range(width)
        ]
        for t in range(width):
            k = first + t
            column = columns[t]
            scale = 1.0 / column[k : k + 1, :]
            weight = jnp.where(rows > k, column * scale, 0.0)
            work = work - weight * work[k : k + 1, :]
            for u in range(t + 1, width):
                columns[u] = columns[u] - weight * column[first + u : first + u + 1, :]
    pivots = jnp.sum(jnp.where(rows == lanes, work, 0.0), axis=1, keepdims=True)
    scaled = work * lax.rsqrt(pivots)
    upper = jnp.where(small_lanes >= small_rows, scaled[:, :B], 0.0)
    inverse = jnp.where(small_lanes <= small_rows, scaled[:, B:], 0.0)
    return upper, inverse


FAR_FIRST = [10, 6, 14, 9, 11, 2, 8, 5, 7, 13, 15, 1, 3, 4, 12]


def pack(block):
    return jnp.concatenate([block[:HALF], block[HALF:]], axis=1)


def unpack(block):
    return jnp.concatenate([block[:, :B], block[:, B:]], axis=0)


def lanczos_kernel(
    start_ref,
    hi_ref,
    mid_ref,
    low_ref,
    basis_ref,
    diag_ref,
    off_ref,
    tile_hi,
    tile_mid,
    tile_low,
    work,
    current,
    applied,
    gathered,
    stacked,
    partial,
    landed,
    gram,
    stage1,
    slab,
    stage2,
    total,
    full,
    tile_sem,
    send_q,
    recv_q,
    send_p,
    recv_p,
    send_1,
    recv_1,
    send_2,
    recv_2,
    send_3,
    recv_3,
):
    tm = lax.axis_index("tm")
    panel = lax.axis_index("panel")
    low_z = tm // PLANE
    plane = tm % PLANE
    line = low_z * 4 + panel
    tiles = [
        pltpu.make_async_copy(source, target, tile_sem.at[at])
        for at, (source, target) in enumerate(
            ((hi_ref, tile_hi), (mid_ref, tile_mid), (low_ref, tile_low))
        )
    ]
    for copy in tiles:
        copy.start()

    plane_peer = peers(plane, low_z, panel)

    def line_peer(step):
        spot_z = (low_z + step // 4) % 2
        spot_p = (panel + step % 4) % 4
        return spot_z * 4 + spot_p, (spot_z * PLANE + plane, spot_p)

    barrier = pltpu.get_barrier_semaphore()
    for step in range(1, PLANE):
        pl.semaphore_signal(barrier, inc=1, device_id=plane_peer(step)[1], device_id_type=MESH)
    for step in range(1, LINE):
        pl.semaphore_signal(barrier, inc=1, device_id=line_peer(step)[1], device_id_type=MESH)
    pl.semaphore_wait(barrier, PLANE + LINE - 2)

    def remote(source, target, send, receive, device):
        return pltpu.make_async_remote_copy(
            src_ref=source,
            dst_ref=target,
            send_sem=send,
            recv_sem=receive,
            device_id=device,
            device_id_type=MESH,
        )

    work[...] = start_ref[...]
    current[...] = jnp.zeros_like(current)
    applied[...] = jnp.zeros_like(applied)

    def one_step(step_at, last):
        slot = step_at % 2
        before = current[...]
        rows_block = work[...]

        moved = []

        def part_at(spot, color):
            return gathered.at[slot, spot, pl.ds(40 * color, 40 - 8 * color)]

        def spot_at(turn_x, turn_y):
            return ((plane // 4 + turn_x) % 4) * 4 + (plane % 4 + turn_y) % 4

        def forward(origin_x, origin_y, color, along, to_turn):
            to_x, to_y = (to_turn, 0) if along == 0 else (0, to_turn)
            part = part_at(spot_at(4 - origin_x, 4 - origin_y), color)
            key = (origin_x + to_x) % 4 * 4 + (origin_y + to_y) % 4
            copy = remote(
                part,
                part,
                send_q.at[color, key],
                recv_q.at[slot, color, key],
                (low_z * PLANE + spot_at(to_x, to_y), panel),
            )
            copy.start()
            moved.append(copy)

        def await_part(origin_x, origin_y, color):
            key = origin_x * 4 + origin_y
            part = part_at(spot_at(4 - origin_x, 4 - origin_y), color)
            remote(
                part, part, send_q.at[color, key], recv_q.at[slot, color, key], (tm, panel)
            ).wait_recv()

        if not last:
            gathered[slot, plane] = pack(rows_block)
            for turn in (2, 1, 3):
                forward(0, 0, 0, 0, turn)
                forward(0, 0, 1, 1, turn)
            for turn in (2, 1, 3):
                forward(0, 0, 0, 1, turn)
                forward(0, 0, 1, 0, turn)

        both = jnp.concatenate([before, rows_block], axis=1)
        gram[...] = exact_dot(both, both, ((0,), (0,))).reshape(LINE, 16, 2 * B)
        firsts = [
            remote(
                gram.at[line_peer(step)[0]],
                stage1.at[line],
                send_1.at[step],
                recv_1.at[step],
                line_peer(step)[1],
            )
            for step in range(1, LINE)
        ]
        for copy in firsts:
            copy.start()
        stage1[line] = gram[line]

        def lay(spot, block):
            hi, mid, low = split3(unpack(block))
            at = pl.ds(pl.multiple_of(spot * ROWS, ROWS), ROWS)
            stacked[at, :] = jnp.concatenate([hi, mid, low], axis=1)

        wave = (1, 3, 2)
        if not last:
            lay(plane, gathered[slot, plane])
            for turn in wave:
                await_part(turn, 0, 0)
                for to_turn in (2, 1, 3):
                    forward(turn, 0, 0, 1, to_turn)
                await_part(0, turn, 1)
                for to_turn in (2, 1, 3):
                    forward(0, turn, 1, 0, to_turn)
        for copy in firsts:
            copy.wait()
        reduced = stage1[0]
        for spot in range(1, LINE):
            reduced = reduced + stage1[spot]
        slab[...] = reduced
        stage2[slot, plane] = reduced
        seconds = [
            remote(
                slab,
                stage2.at[slot, plane],
                send_2.at[step],
                recv_2.at[slot, step],
                plane_peer(step)[1],
            )
            for step in FAR_FIRST
        ]
        for copy in seconds:
            copy.start()

        sums = [
            remote(
                partial.at[line_peer(step)[0]],
                landed.at[slot, line],
                send_p.at[step],
                recv_p.at[slot, step],
                line_peer(step)[1],
            )
            for step in range(1, LINE)
            if not last
        ]

        def multiply(h):
            first = jnp.dot(tile_hi[h], stacked[...], preferred_element_type=jnp.float32)
            second = jnp.dot(
                tile_mid[h], stacked[:, : 2 * B], preferred_element_type=jnp.float32
            )
            third = jnp.dot(tile_low[h], stacked[:, :B], preferred_element_type=jnp.float32)
            low_part = third + second[:, B:] + first[:, 2 * B :]
            return first[:, :B] + (first[:, B : 2 * B] + second[:, :B] + low_part)

        def send_sums(h):
            for at, copy in enumerate(sums):
                @pl.when((low_z + (at + 1) // 4) % 2 == h)
                def _():
                    copy.start()

            @pl.when(low_z == h)
            def _():
                landed[slot, line] = partial[line]

        def finish(h):
            product = multiply(h)
            for spot in range(4):
                rows = product[spot * ROWS : (spot + 1) * ROWS]
                partial[h * 4 + spot] = pack(rows)
            send_sums(h)

        def place(origin_x, origin_y):
            spot = spot_at(4 - origin_x, 4 - origin_y)
            lay(spot, gathered[slot, spot])

        if not last:
            for turn in wave:
                await_part(0, turn, 0)
                await_part(turn, 0, 1)
                place(0, turn)
                place(turn, 0)
            for turn_x in wave:
                for turn_y in wave:
                    await_part(turn_x, turn_y, 0)
                    await_part(turn_x, turn_y, 1)
                    place(turn_x, turn_y)

            @pl.when(step_at == 0)
            def _():
                for copy in tiles:
                    copy.wait()

            finish(0)

        for copy in seconds:
            copy.wait()
        reduced = stage2[slot, 0]
        for spot in range(1, PLANE):
            reduced = reduced + stage2[slot, spot]
        total[...] = reduced
        full[line] = reduced
        thirds = [
            remote(total, full.at[line], send_3.at[step], recv_3.at[step], line_peer(step)[1])
            for step in range(1, LINE)
        ]
        for copy in thirds:
            copy.start()
        if not last:
            finish(1)
        for copy in thirds:
            copy.wait()
        summed = full[...].reshape(2 * B, 2 * B)
        basis_gram = summed[:B, :B]
        diagonal = summed[:B, B:]
        work_gram = summed[B:, B:]
        weighted = exact_dot(basis_gram, diagonal, ((1,), (0,)))
        left = exact_dot(diagonal, 2.0 * diagonal - weighted, ((0,), (0,)))
        upper, inverse = factor(work_gram - left)
        diag_ref[jnp.maximum(step_at - 1, 0)] = diagonal
        off_ref[step_at] = upper
        if last:
            reduced = rows_block - exact_dot(before, diagonal, ((1,), (0,)))
            basis_ref[step_at] = exact_dot(reduced, inverse, ((1,), (1,)))
            return
        for copy in sums:
            copy.wait()
        for copy in moved:
            copy.wait_send()
        value = landed[slot, 0]
        for spot in range(1, LINE):
            value = value + landed[slot, spot]
        old = jnp.concatenate([before, applied[...]], axis=0)
        new = jnp.concatenate([rows_block, unpack(value)], axis=0)
        reduced = new - exact_dot(old, diagonal, ((1,), (0,)))
        fresh = exact_dot(reduced, inverse, ((1,), (1,)))
        basis_ref[step_at] = fresh[:ROWS]
        current[...] = fresh[:ROWS]
        applied[...] = fresh[ROWS:]
        work[...] = fresh[ROWS:] - exact_dot(before, upper, ((1,), (1,)))

    def body(step_at, carry):
        one_step(step_at, False)
        return carry

    lax.fori_loop(0, ITERS, body, 0)
    one_step(ITERS, True)


def lanczos(start, hi, mid, low):
    vmem = pl.BlockSpec(memory_space=pltpu.VMEM)
    away = pl.BlockSpec(memory_space=pl.ANY)
    dma = pltpu.SemaphoreType.DMA
    tile = pltpu.VMEM((2, 4 * ROWS, COLS), jnp.bfloat16)
    return pl.pallas_call(
        lanczos_kernel,
        out_shape=(
            jax.ShapeDtypeStruct((ITERS + 1, ROWS, B), jnp.float32),
            jax.ShapeDtypeStruct((ITERS, B, B), jnp.float32),
            jax.ShapeDtypeStruct((ITERS + 1, B, B), jnp.float32),
        ),
        in_specs=[vmem, away, away, away],
        out_specs=(vmem, vmem, vmem),
        scratch_shapes=[
            tile,
            tile,
            tile,
            pltpu.VMEM((ROWS, B), jnp.float32),
            pltpu.VMEM((ROWS, B), jnp.float32),
            pltpu.VMEM((ROWS, B), jnp.float32),
            pltpu.VMEM((2, PLANE, HALF, 2 * B), jnp.float32),
            pltpu.VMEM((COLS, 3 * B), jnp.bfloat16),
            pltpu.VMEM((LINE, HALF, 2 * B), jnp.float32),
            pltpu.VMEM((2, LINE, HALF, 2 * B), jnp.float32),
            pltpu.VMEM((LINE, 16, 2 * B), jnp.float32),
            pltpu.VMEM((LINE, 16, 2 * B), jnp.float32),
            pltpu.VMEM((16, 2 * B), jnp.float32),
            pltpu.VMEM((2, PLANE, 16, 2 * B), jnp.float32),
            pltpu.VMEM((16, 2 * B), jnp.float32),
            pltpu.VMEM((LINE, 16, 2 * B), jnp.float32),
            dma((3,)),
            dma((2, PLANE)),
            dma((2, 2, PLANE)),
            dma((LINE,)),
            dma((2, LINE)),
            dma((LINE,)),
            dma((LINE,)),
            dma((PLANE,)),
            dma((2, PLANE)),
            dma((LINE,)),
            dma((LINE,)),
        ],
        compiler_params=pltpu.CompilerParams(
            collective_id=0, has_side_effects=True, vmem_limit_bytes=60 * 1024 * 1024
        ),
    )(start, hi, mid, low)


def hand_over_kernel(basis_ref, diag_ref, off_ref, basis_out, diag_out, off_out):
    basis_out[...] = basis_ref[...]
    diag_out[...] = diag_ref[...]
    off_out[...] = off_ref[...]


def hand_over(*arrays):
    vmem = pl.BlockSpec(memory_space=pltpu.VMEM)
    return pl.pallas_call(
        hand_over_kernel,
        out_shape=tuple(jax.ShapeDtypeStruct(x.shape, x.dtype) for x in arrays),
        in_specs=[vmem] * 3,
        out_specs=(vmem, vmem, vmem),
    )(*arrays)


def local(series, start_block):
    covariance, hi, mid, low = assemble(lag_blocks(series))
    basis, diag, off = hand_over(*lanczos(start_block, hi, mid, low))
    return covariance, basis, diag, off


def solution(mesh):
    placed = (P(None, "tm"), P(("tm", "panel"), None))
    return jax.shard_map(
        local,
        mesh=mesh,
        in_specs=placed,
        out_specs=(P(("tm", "panel"), None), P(None, ("tm", "panel"), None), P(), P()),
        check_vma=False,
    )
```
